512 devices in a mesh: dp: 32 (over x, z), patch: 16 (over y, core).
Axes of the slice: x: 4, y: 8, z: 8, core: 2. Of those that a mesh axis runs over, the one named last changes fastest.
Arguments:
- query_rows: bfloat16 [32, 2048, 576], P('dp', 'patch'), may hold values from -6 to 6
- key_rows: bfloat16 [32, 2048, 576], P('dp', 'patch'), may hold values from -6 to 6
- value_rows: bfloat16 [32, 2048, 576], P('dp', 'patch'), may hold values from -6 to 6
- out_weight: bfloat16 [576, 1152], replicated, may hold values from -0.25 to 0.25
- target: bfloat16 [32, 2048, 1152], P('dp', 'patch'), may hold values from -6 to 6
- lengths: int32 [32], P('dp'), may hold values from 256 to 2048
- segments: int32 [32, 2048], P('dp', 'patch'), may hold values from 0 to 7, never falling along the last dimension, each value on 1 to 1024 neighbouring positions
Outputs:
- query_grad: float32 [32, 2048, 576], P('dp', 'patch')
- key_grad: float32 [32, 2048, 576], P('dp', 'patch')
- value_grad: float32 [32, 2048, 576], P('dp', 'patch')
- weight_grad: float32 [576, 1152], P('patch', 'dp')
- loss: float32 [], replicated
The draws below stay inside these ranges and needn't reach their ends.
All inputs are finite; a program needn't handle non-finite values.
Results may differ from the reference program's by a relative error of at most 0.024.
Values may be sent and summed in bfloat16 or wider, within the bound.
No kernel may reach another device: no remote copies, remote signals or barrier semaphores. Data moves between devices by JAX's collectives and lax.ppermute only.
A program may use at most 64 MiB of HBM per device.

```python
import math
import jax
import jax.numpy as jnp
import numpy as np
from jax import lax

WIDTH = 1152
HEADS = 8
HEAD_DIM = 72
TOK_DEV = 128
FEAT = 576
SEQ = 2048
SAMPLES = 32


def draw_rows(key, salt, chosen_rows):
    fresh_key = jax.random.fold_in(key, salt)
    sampled = jnp.clip(1.5 * jax.random.normal(fresh_key, (SAMPLES, SEQ, FEAT), jnp.float32), -6.0, 6.0)
    return sampled.astype(jnp.bfloat16)


def draw_query_rows(key, part):
    positions = jnp.arange(SEQ)
    return draw_rows(key, 1, positions % TOK_DEV == 0)


def draw_key_rows(key, part):
    positions = jnp.arange(SEQ)
    return draw_rows(key, 2, positions % TOK_DEV == 0)


def plant(entries, key, low, largest):
    longest = entries.shape.index(max(entries.shape))
    spots = []
    for shift in (0, 1):
        where = [jax.random.randint(jax.random.fold_in(key, axis), (), 0, length) for axis, length in enumerate(entries.shape)]
        where[longest] = (where[longest] + shift) % entries.shape[longest]
        spots.append(tuple(where))
    return entries.at[spots[0]].set(low).at[spots[1]].set(largest)


def steps_of(stream_key, extent, split, least, largest):
    level = 1.0
    for position, shards_of in split:
        heights = jax.random.uniform(jax.random.fold_in(jax.random.fold_in(stream_key, 6), position), (shards_of,), jnp.float32, least / len(split), largest / len(split))
        level = level * jnp.repeat(jnp.exp(heights), extent[position] // shards_of).reshape((-1,) + (1,) * (len(extent) - 1 - position))
    return level


def profile(count, total, most, skew):
    weights = [(1 << 20) // math.isqrt(rank ** skew) + 1 for rank in range(2, count + 1)]
    surplus, counts = total - most - (count - 1), [1] * (count - 1)
    while surplus > 0:
        candidates = [i for i in range(count - 1) if counts[i] < most]
        pool, remaining = sum([weights[i] for i in candidates]), surplus
        for i in candidates:
            more = min(most - counts[i], max(1, remaining * weights[i] // pool), surplus)
            counts[i] = counts[i] + more
            surplus = surplus - more
    return np.array([most] + counts)


def uneven_parts(key, number_of, total, most, skew):
    if number_of == 2:
        one = jax.random.randint(key, (), max(1, total - most), min(most, total - 1) + 1)
        return jnp.stack([one, total - one])
    tallies = jnp.asarray(profile(number_of, total, most, skew), jnp.int32)
    pairs = (number_of - 1) // 2
    donor, sink = tallies[1:1 + 2 * pairs:2], tallies[2:2 + 2 * pairs:2]
    slack = jnp.minimum(donor - 1, most - sink)
    shifted = jax.random.randint(jax.random.fold_in(key, 1), (pairs,), 0, 1 << 20) % (slack + 1)
    tallies = tallies.at[1:1 + 2 * pairs:2].set(donor - shifted).at[2:2 + 2 * pairs:2].set(sink + shifted)
    return tallies[jax.random.permutation(jax.random.fold_in(key, 2), number_of)]


def normal_values(rng, shape, spread, most, split=(), kind=jnp.bfloat16):
    array = spread * jax.random.normal(rng, shape, jnp.float32)
    if split:
        array = array * steps_of(rng, shape, split, -0.22, 0.18)
    return jnp.clip(array, -most, most).astype(kind)


def setup_inputs(seed: int = 0) -> dict:
    arg_keys = jax.random.split(jax.random.key(seed), 8)
    query_rows = draw_query_rows(jax.random.fold_in(arg_keys[7], 71), 0)
    key_rows = draw_key_rows(jax.random.fold_in(arg_keys[7], 71), 0)
    value_rows = normal_values(arg_keys[2], (SAMPLES, SEQ, FEAT), 1.0, 6.0, ((0, 32), (1, 16)))
    out_weight = normal_values(arg_keys[3], (FEAT, WIDTH), FEAT ** -0.5, 0.25)
    target = normal_values(arg_keys[4], (SAMPLES, SEQ, WIDTH), 1.0, 6.0, ((0, 32), (1, 16)))
    lengths = plant(jax.random.randint(arg_keys[5], (SAMPLES,), SEQ // 8, SEQ + 1), jax.random.fold_in(arg_keys[5], 1), SEQ // 8, SEQ).astype(jnp.int32)
    segments = jax.vmap(lambda own: jnp.searchsorted(jnp.cumsum(uneven_parts(own, 8, SEQ, SEQ // 2, 2)), jnp.arange(SEQ), side="right"))(jax.random.split(arg_keys[6], SAMPLES)).reshape((SAMPLES, SEQ)).astype(jnp.int32)
    return {"query_rows": query_rows, "key_rows": key_rows, "value_rows": value_rows, "out_weight": out_weight, "target": target, "lengths": lengths, "segments": segments}


NEG_LARGE = -1e+30

def widen(value):
    return lax.optimization_barrier(value).astype(jnp.float32)

def one_sample(packed, out_weight):
    query_rows, key_rows, value_rows, target_rows, length, segment_row = packed
    score_scale = 1.0 / math.sqrt(HEAD_DIM)
    query_heads = query_rows.astype(jnp.float32).reshape(SEQ, HEADS, HEAD_DIM)
    key_heads = key_rows.astype(jnp.float32).reshape(SEQ, HEADS, HEAD_DIM)
    value_heads = value_rows.astype(jnp.float32).reshape(SEQ, HEADS, HEAD_DIM)
    live = lax.iota(jnp.int32, SEQ) < length
    group = jnp.where(live, segment_row, -1)
    allowed = (group[:, None] == group[None, :])[None, :, :]
    scores = jnp.einsum('qhe,khe->hqk', query_heads, key_heads) * score_scale
    masked = jnp.where(allowed, scores, NEG_LARGE)
    row_max = lax.optimization_barrier(jnp.max(masked, axis=2))
    probs = jnp.where(allowed, jnp.exp(masked - row_max[:, :, None]), 0.0)
    denom = lax.optimization_barrier(jnp.sum(probs, axis=2))
    weights = widen(probs.astype(jnp.bfloat16))
    accum = jnp.einsum('hqk,khe->qhe', weights, value_heads)
    attn = (accum / denom.T[:, :, None]).reshape(SEQ, FEAT).astype(jnp.bfloat16)
    log_norm = row_max + jnp.log(denom)
    output = jnp.dot(attn, out_weight, preferred_element_type=jnp.float32)
    error = jnp.where(live[:, None], output - target_rows.astype(jnp.float32), 0.0)
    grad_out = (2.0 * error).astype(jnp.bfloat16)
    attn_wide = widen(attn)
    grad_wide = widen(grad_out)
    weight_part = jnp.einsum('tf,td->fd', attn_wide, grad_wide)
    grad_attn = jnp.einsum('td,fd->tf', grad_wide, out_weight.astype(jnp.float32)).astype(jnp.bfloat16)
    grad_attn_wide = widen(grad_attn)
    delta = lax.optimization_barrier(jnp.sum((grad_attn_wide * attn_wide).reshape(SEQ, HEADS, HEAD_DIM), axis=2)).T
    back_probs = jnp.where(allowed, jnp.exp(masked - log_norm[:, :, None]), 0.0)
    grad_heads = grad_attn_wide.reshape(SEQ, HEADS, HEAD_DIM)
    dprobs = jnp.einsum('qhe,khe->hqk', grad_heads, value_heads)
    dscores = widen((back_probs * (dprobs - delta[:, :, None])).astype(jnp.bfloat16))
    query_raw = jnp.einsum('hqk,khe->qhe', dscores, key_heads) * score_scale
    key_raw = jnp.einsum('hqk,qhe->khe', dscores, query_heads) * score_scale
    back_weights = widen(back_probs.astype(jnp.bfloat16))
    value_raw = jnp.einsum('hqk,qhe->khe', back_weights, grad_heads)
    return (query_raw.reshape(SEQ, FEAT), key_raw.reshape(SEQ, FEAT), value_raw.reshape(SEQ, FEAT), weight_part, jnp.sum(error * error))

def reference(query_rows, key_rows, value_rows, out_weight, target, lengths, segments):

    def per_sample(packed):
        return one_sample(packed, out_weight)
    results = lax.map(per_sample, (query_rows, key_rows, value_rows, target, lengths, segments))
    count = jnp.sum(lengths).astype(jnp.float32)
    ratio = jnp.float32(SAMPLES * SEQ) / count
    query_grad = ratio * results[0]
    key_grad = ratio * results[1]
    value_grad = ratio * results[2]
    weight_grad = lax.optimization_barrier(jnp.sum(results[3], axis=0)) * (ratio / SEQ)
    loss = jnp.sum(results[4]) / (count * WIDTH)
    return (query_grad, key_grad, value_grad, weight_grad, loss)
```

```python
import math

import jax
import jax.numpy as jnp
from jax import lax
from jax.experimental import pallas as pl
from jax.experimental.pallas import tpu as pltpu
from jax.sharding import Mesh
from jax.sharding import PartitionSpec as P

WIDTH = 1152
HEADS = 8
HD = 72
TOK = 128
FEAT = 576
SEQ = 2048
SAMPLES = 32
CHIPS = 8
PATCHES = 16
COLS = WIDTH // SAMPLES
ROWS = FEAT // PATCHES
PAD = 40
LANES = 640
BUF = 3 * HD + 8
QB = 256
NEG_LARGE = -1e30
SCALE = 1.0 / math.sqrt(HD)
EXP2_SCALE = SCALE * math.log2(math.e)
PATCH = ("patch_0", "patch_1")
DP = ("dp_0", "dp_1")
F32 = jnp.float32
BF16 = jnp.bfloat16

VM = pl.BlockSpec(memory_space=pltpu.VMEM)
SM = pl.BlockSpec(memory_space=pltpu.SMEM)


def call(kernel, name, out_shape, in_specs, flops, nbytes, scratch=(), out_specs=None):
    return pl.pallas_call(
        kernel,
        name=name,
        out_shape=out_shape,
        in_specs=in_specs,
        out_specs=out_specs if out_specs is not None else jax.tree.map(lambda _: VM, out_shape),
        scratch_shapes=list(scratch),
        cost_estimate=pl.CostEstimate(flops=flops, bytes_accessed=nbytes, transcendentals=0),
        compiler_params=pltpu.CompilerParams(vmem_limit_bytes=40 * 1024 * 1024),
    )


def dot(a, b, dims):
    return lax.dot_general(a, b, (dims, ((), ())), preferred_element_type=F32)


NN = ((1,), (0,))
NT = ((1,), (1,))


def pack_kernel(q_ref, k_ref, v_ref, seg_ref, out_ref):
    for at, ref in enumerate((q_ref, k_ref, v_ref)):
        for h in range(HEADS):
            out_ref[h, at * HD : (at + 1) * HD, :] = ref[0, h * HD : (h + 1) * HD, :]
    seg = jnp.broadcast_to(seg_ref[...].astype(F32), (8, TOK)).astype(BF16)
    for h in range(HEADS):
        out_ref[h, 3 * HD : BUF, :] = seg


def group_rows(ref, chip, core, length):
    seg = ref[chip, 3 * HD : BUF, :].astype(F32)[0:1]
    at = (2 * chip + core) * TOK + lax.broadcasted_iota(jnp.int32, (1, TOK), 1)
    return jnp.where(at < length, seg, -1.0)


def columns(ref, at):
    return jnp.concatenate([ref[c, at : at + HD, :] for c in range(CHIPS)], axis=1)


def forward_kernel(len_ref, own_ref, other_ref, attn_ref, probs_ref, inv_ref, key_sc, group_sc, value_sc):
    core = lax.axis_index("patch_1")
    length = len_ref[0]
    own_groups = []
    for side, ref in enumerate((own_ref, other_ref)):
        for c in range(CHIPS):
            at = (side * CHIPS + c) * TOK
            key_sc[at : at + TOK, :] = ref[c, HD : 2 * HD, :].astype(F32).T.astype(BF16)
            value_sc[:, at : at + TOK] = ref[c, 2 * HD : 3 * HD, :]
            group = group_rows(ref, c, core if side == 0 else 1 - core, length)
            if side == 0:
                own_groups.append(group)
            group_sc[at : at + TOK, :] = jnp.broadcast_to(group, (TOK, TOK)).T
    for b in range(SEQ // 2 // QB):
        pair = QB // TOK
        query = jnp.concatenate([own_ref[b * pair + i, 0:HD, :] for i in range(pair)], axis=1)
        group = jnp.concatenate([own_groups[b * pair + i] for i in range(pair)], axis=1)
        scores = dot(key_sc[...], query, NN)
        key_group = jnp.concatenate([group_sc[...]] * pair, axis=1)
        masked = jnp.where(key_group == group, scores, NEG_LARGE)
        top = jnp.max(masked, axis=0, keepdims=True)
        probs = jnp.exp2((masked - top) * EXP2_SCALE)
        inv = 1.0 / jnp.sum(probs, axis=0, keepdims=True)
        weights = probs.astype(BF16)
        probs_ref[b] = weights
        attn = (dot(value_sc[...], weights, NN) * inv).astype(BF16)
        inv_ref[b : b + 1, :] = inv
        for i in range(pair):
            attn_ref[b * pair + i] = attn[:, i * TOK : (i + 1) * TOK]


def project_kernel(len_ref, attn_ref, weight_ref, target_ref, back_ref, out_ref, loss_ref):
    place = 2 * lax.axis_index("patch_0") + lax.axis_index("patch_1")
    attn = attn_ref[...].reshape(FEAT, TOK).astype(F32).T.astype(BF16)
    output = dot(attn, weight_ref[...], NN)
    at = place * TOK + lax.broadcasted_iota(jnp.int32, (TOK, WIDTH), 0)
    error = jnp.where(at < len_ref[0], output - target_ref[0].astype(F32), 0.0)
    grad_out = (2.0 * error).astype(BF16)
    out_ref[...] = grad_out
    loss_ref[...] = jnp.sum(error * error, axis=0, keepdims=True)
    back = dot(weight_ref[...], grad_out, NT).astype(BF16)
    for h in range(HEADS):
        back_ref[h] = back[h * HD : (h + 1) * HD, :]


def high_low(value):
    high = value.astype(BF16).astype(F32)
    return high, value - high


def weight_kernel(len_ref, attn_ref, grad_ref, loss_ref, out_ref, acc):
    attn = attn_ref[...].reshape(FEAT, TOK)
    turned = grad_ref[...].astype(F32).T.astype(BF16)
    acc[...] = dot(turned, attn, NT)
    length = len_ref[0]
    upper = length // 256
    lower = length - upper * 256
    loss = jnp.broadcast_to(jnp.sum(loss_ref[...], axis=1, keepdims=True), (1, LANES))
    loss_high, loss_low = high_low(loss)
    rows = jnp.concatenate(
        [
            jnp.full((1, LANES), upper.astype(F32)),
            jnp.full((1, LANES), lower.astype(F32)),
            loss_high,
            loss_low,
        ],
        axis=0,
    )
    tail = jnp.zeros((PAD, LANES - FEAT), BF16)
    for d in range(SAMPLES):
        block = jnp.concatenate([acc[d * COLS : (d + 1) * COLS, :], rows[:, :FEAT]], axis=0)
        out_ref[d, :, 0:FEAT] = block.astype(BF16)
        out_ref[d, :, FEAT:LANES] = tail


def backward_kernel(own_ref, other_ref, attn_ref, back_ref, probs_ref, inv_ref, query_out, own_out, other_out, value_sc, key_sc, key_acc, value_acc):
    for side, ref in enumerate((own_ref, other_ref)):
        for c in range(CHIPS):
            at = (side * CHIPS + c) * TOK
            value_sc[at : at + TOK, :] = ref[c, 2 * HD : 3 * HD, :].astype(F32).T.astype(BF16)
            key_sc[:, at : at + TOK] = ref[c, HD : 2 * HD, :]
    for b in range(SEQ // 2 // QB):
        pair = QB // TOK
        chips = range(b * pair, (b + 1) * pair)
        query = jnp.concatenate([own_ref[c, 0:HD, :] for c in chips], axis=1)
        attn = jnp.concatenate([attn_ref[c] for c in chips], axis=1)
        back = jnp.concatenate([back_ref[c] for c in chips], axis=1)
        back = (back.astype(F32) * inv_ref[b : b + 1, :]).astype(BF16)
        delta = jnp.sum(back.astype(F32) * attn.astype(F32), axis=0, keepdims=True)
        probs = probs_ref[b]
        dprobs = dot(value_sc[...], back, NN)
        dscores = (probs.astype(F32) * (dprobs - delta)).astype(BF16)
        query_grad = dot(key_sc[...], dscores, NN).astype(BF16)
        for i, c in enumerate(chips):
            query_out[c] = query_grad[:, i * TOK : (i + 1) * TOK]
        key_part = dot(query, dscores, NT)
        value_part = dot(back, probs, NT)
        if b == 0:
            key_acc[...] = key_part
            value_acc[...] = value_part
        else:
            key_acc[...] += key_part
            value_acc[...] += value_part
    for side, ref in enumerate((own_out, other_out)):
        for c in range(CHIPS):
            at = (side * CHIPS + c) * TOK
            ref[c, 0:HD, :] = key_acc[:, at : at + TOK].astype(BF16)
            ref[c, HD : 2 * HD, :] = value_acc[:, at : at + TOK].astype(BF16)


def join_kernel(query_ref, own_ref, other_ref, out_ref):
    out_ref[:, 0:HD, :] = query_ref[...]
    out_ref[:, HD : 3 * HD, :] = (own_ref[...].astype(F32) + other_ref[...].astype(F32)).astype(BF16)


def reduce_kernel(part_ref, out_ref, stat_ref):
    total = part_ref[0].astype(F32)
    for d in range(1, SAMPLES):
        total = total + part_ref[d].astype(F32)
    count = 256.0 * total[COLS : COLS + 1, 0:TOK] + total[COLS + 1 : COLS + 2, 0:TOK]
    loss = total[COLS + 2 : COLS + 3, 0:TOK] + total[COLS + 3 : COLS + 4, 0:TOK]
    stat_ref[...] = jnp.broadcast_to(count, (8, TOK))
    loss_high, loss_low = high_low(loss)
    turned = jnp.concatenate([total, jnp.zeros((TOK - PAD, LANES), F32)], axis=0).T
    tail = jnp.concatenate([loss_high, loss_low, jnp.zeros((PAD - ROWS - 2, TOK), F32)], axis=0)
    for p in range(PATCHES):
        out_ref[p] = jnp.concatenate([turned[p * ROWS : (p + 1) * ROWS, :], tail], axis=0).astype(BF16)


def unpack_kernel(rows_ref, stat_ref, query_ref, key_ref, value_ref):
    ratio = float(SAMPLES * SEQ) / stat_ref[0:1, :]
    for at, (ref, factor) in enumerate(((query_ref, SCALE), (key_ref, SCALE), (value_ref, 1.0))):
        for h in range(HEADS):
            rows = rows_ref[h, at * HD : (at + 1) * HD, :].astype(F32)
            ref[0, h * HD : (h + 1) * HD, :] = rows * (ratio * factor)


def last_kernel(part_ref, stat_ref, weight_ref, loss_ref):
    total = part_ref[0].astype(F32)
    for p in range(1, PATCHES):
        total = total + part_ref[p].astype(F32)
    count = stat_ref[0:1, :]
    ratio = float(SAMPLES * SEQ) / count
    weight_ref[...] = (total[0:ROWS, :] * (ratio / SEQ))[:, 0:COLS]
    loss_ref[...] = (total[ROWS : ROWS + 1, :] + total[ROWS + 1 : ROWS + 2, :]) / (count * WIDTH)


def exchange(value, axis):
    return lax.all_to_all(value, axis, 0, 0, tiled=True)


def swap(value):
    return lax.ppermute(value, "patch_1", [(0, 1), (1, 0)])


def shape(dims, dtype):
    return jax.ShapeDtypeStruct(dims, dtype)


def local(query_rows, key_rows, value_rows, out_weight, target, lengths, segments):
    buffer = shape((CHIPS, BUF, TOK), BF16)
    heads = shape((CHIPS, HD, TOK), BF16)
    packed = call(pack_kernel, "pack", buffer, [VM] * 4, 10**6, 10**6)(
        *(jnp.swapaxes(rows, 1, 2) for rows in (query_rows, key_rows, value_rows)), segments
    )
    own = exchange(packed, "patch_0")
    other = swap(own)
    blocks = SEQ // 2 // QB
    attn, probs, inv = call(
        forward_kernel,
        "forward",
        (heads, shape((blocks, SEQ, QB), BF16), shape((blocks, QB), F32)),
        [SM, VM, VM],
        4 * HD * SEQ * SEQ // 2,
        6 * 10**6,
        [pltpu.VMEM((SEQ, HD), BF16), pltpu.VMEM((SEQ, TOK), F32), pltpu.VMEM((HD, SEQ), BF16)],
    )(lengths, own, other)
    attn_rows = exchange(attn, "patch_0")
    back, grad_out, loss_part = call(
        project_kernel,
        "project",
        (heads, shape((TOK, WIDTH), BF16), shape((1, WIDTH), F32)),
        [SM, VM, VM, VM],
        4 * TOK * FEAT * WIDTH,
        3 * 10**6,
    )(lengths, attn_rows, out_weight, target)
    back_heads = exchange(back, "patch_0")
    weight_part = call(
        weight_kernel,
        "weight",
        shape((SAMPLES, PAD, LANES), BF16),
        [SM, VM, VM, VM],
        2 * TOK * FEAT * WIDTH,
        3 * 10**6,
        [pltpu.VMEM((WIDTH, FEAT), F32)],
    )(lengths, attn_rows, grad_out, loss_part)
    weight_parts = exchange(weight_part, DP)
    pair = shape((CHIPS, 2 * HD, TOK), BF16)
    query_grad, own_grad, other_grad = call(
        backward_kernel,
        "backward",
        (heads, pair, pair),
        [VM] * 6,
        8 * HD * SEQ * SEQ // 2,
        6 * 10**6,
        [
            pltpu.VMEM((SEQ, HD), BF16),
            pltpu.VMEM((HD, SEQ), BF16),
            pltpu.VMEM((HD, SEQ), F32),
            pltpu.VMEM((HD, SEQ), F32),
        ],
    )(own, other, attn, back_heads, probs, inv)
    got = swap(other_grad)
    joined = call(join_kernel, "join", shape((CHIPS, 3 * HD, TOK), BF16), [VM] * 3, 10**6, 10**6)(
        query_grad, own_grad, got
    )
    grads = exchange(joined, "patch_0")
    reduced, stats = call(
        reduce_kernel,
        "reduce",
        (shape((PATCHES, PAD, TOK), BF16), shape((8, TOK), F32)),
        [VM],
        10**6,
        2 * 10**6,
    )(weight_parts)
    weight_last = exchange(reduced, PATCH)
    rows = shape((1, FEAT, TOK), F32)
    query_out, key_out, value_out = call(
        unpack_kernel, "unpack", (rows, rows, rows), [VM, VM], 10**6, 10**6
    )(grads, stats)
    weight_grad, loss = call(
        last_kernel, "last", (shape((ROWS, COLS), F32), shape((1, TOK), F32)), [VM, VM], 10**5, 10**5
    )(weight_last, stats)
    grads_out = (jnp.swapaxes(rows, 1, 2) for rows in (query_out, key_out, value_out))
    return *grads_out, weight_grad, loss[0, 0]


def solution(mesh):
    torus = Mesh(mesh.devices.reshape(4, 8, 8, 2), ("dp_0", "dp_1", "patch_0", "patch_1"))
    return jax.shard_map(
        local,
        mesh=torus,
        in_specs=(
            P(DP, PATCH, None),
            P(DP, PATCH, None),
            P(DP, PATCH, None),
            P(),
            P(DP, PATCH, None),
            P(DP),
            P(DP, PATCH),
        ),
        out_specs=(P(DP, PATCH, None), P(DP, PATCH, None), P(DP, PATCH, None), P(PATCH, DP), P()),
        check_vma=False,
    )
```

```python
import math

import jax
import jax.numpy as jnp
from jax import lax
from jax.experimental import pallas as pl
from jax.experimental.pallas import tpu as pltpu
from jax.sharding import Mesh
from jax.sharding import PartitionSpec as P


WIDTH = 1152
HEADS = 8
HD = 72
TOK = 128
FEAT = 576
SEQ = 2048
SAMPLES = 32
CHIPS = 8
PATCHES = 16
COLS = WIDTH // SAMPLES
ROWS = FEAT // PATCHES
HALF = FEAT // 2
STAT = COLS * HALF // TOK
PAD = 88
LAST = ROWS + 4
PAIR = WIDTH + HALF + 8
BUF = 3 * HD + 8
QB = 256
NEG_LARGE = -1e30
SCALE = 1.0 / math.sqrt(HD)
EXP2_SCALE = SCALE * math.log2(math.e)
PATCH = ("patch_0", "patch_1")
DP = ("dp_0", "dp_1")
F32 = jnp.float32
BF16 = jnp.bfloat16

VM = pl.BlockSpec(memory_space=pltpu.VMEM)
SM = pl.BlockSpec(memory_space=pltpu.SMEM)
HB = pl.BlockSpec(memory_space=pltpu.HBM)
ANY = pl.BlockSpec(memory_space=pl.ANY)


def call(kernel, out_shape, in_specs, flops, nbytes, scratch=(), limit=16, outs=None, aliases=None):
    return pl.pallas_call(
        kernel,
        out_shape=out_shape,
        in_specs=in_specs,
        out_specs=outs if outs is not None else jax.tree.map(lambda _: VM, out_shape),
        scratch_shapes=list(scratch),
        input_output_aliases=aliases or {},
        cost_estimate=pl.CostEstimate(flops=flops, bytes_accessed=nbytes, transcendentals=0),
        compiler_params=pltpu.CompilerParams(vmem_limit_bytes=limit * 1024 * 1024),
    )


def dot(a, b, dims):
    return lax.dot_general(a, b, (dims, ((), ())), preferred_element_type=F32)


NN = ((1,), (0,))
NT = ((1,), (1,))


def pack_kernel(q_ref, k_ref, v_ref, seg_ref, out_ref, seg_sc, sems):
    copies = [
        pltpu.make_async_copy(ref, out_ref.at[:, at * HD : (at + 1) * HD, :], sems.at[at])
        for at, ref in enumerate((q_ref, k_ref, v_ref))
    ]
    copies.append(pltpu.make_async_copy(seg_ref, seg_sc, sems.at[3]))
    for copy in copies:
        copy.start()
    copies[3].wait()
    seg = jnp.broadcast_to(seg_sc[...].astype(F32), (8, TOK)).astype(BF16)
    for h in range(HEADS):
        out_ref[h, 3 * HD : BUF, :] = seg
    for copy in copies[:3]:
        copy.wait()


def group_rows(ref, chip, core, length):
    seg = ref[chip, 3 * HD : BUF, :].astype(F32)[0:1]
    at = (2 * chip + core) * TOK + lax.broadcasted_iota(jnp.int32, (1, TOK), 1)
    return jnp.where(at < length, seg, -1.0)


def forward_kernel(
    len_ref, own_ref, other_ref, attn_ref, probs_ref, inv_ref, key_sc, group_sc, value_sc, probs_sc, sems
):
    core = lax.axis_index("patch_1")
    length = len_ref[0]
    own_groups = []
    copies = []
    for side, ref in enumerate((own_ref, other_ref)):
        for c in range(CHIPS):
            at = (side * CHIPS + c) * TOK
            key_sc[at : at + TOK, :] = ref[c, HD : 2 * HD, :].astype(F32).T.astype(BF16)
            value_sc[:, at : at + TOK] = ref[c, 2 * HD : 3 * HD, :]
            group = group_rows(ref, c, core if side == 0 else 1 - core, length)
            if side == 0:
                own_groups.append(group)
            group_sc[at : at + TOK, :] = jnp.broadcast_to(group, (TOK, TOK)).T
    for b in range(SEQ // 2 // QB):
        pair = QB // TOK
        query = jnp.concatenate([own_ref[b * pair + i, 0:HD, :] for i in range(pair)], axis=1)
        group = jnp.concatenate([own_groups[b * pair + i] for i in range(pair)], axis=1)
        scores = dot(key_sc[...], query, NN)
        key_group = jnp.concatenate([group_sc[...]] * pair, axis=1)
        masked = jnp.where(key_group == group, scores, NEG_LARGE)
        top = jnp.max(masked, axis=0, keepdims=True)
        probs = jnp.exp2((masked - top) * EXP2_SCALE)
        inv = 1.0 / jnp.sum(probs, axis=0, keepdims=True)
        weights = probs.astype(BF16)
        probs_sc[b] = weights
        copies.append(pltpu.make_async_copy(probs_sc.at[b], probs_ref.at[b], sems.at[b]))
        copies[b].start()
        attn = (dot(value_sc[...], weights, NN) * inv).astype(BF16)
        inv_ref[b : b + 1, :] = inv
        for i in range(pair):
            attn_ref[b * pair + i] = attn[:, i * TOK : (i + 1) * TOK]
    for copy in copies:
        copy.wait()


def high_low(value):
    high = value.astype(BF16).astype(F32)
    return high, value - high


def project_kernel(len_ref, attn_ref, weight_ref, target_ref, back_ref, out_ref, loss_ref):
    place = 2 * lax.axis_index("patch_0") + lax.axis_index("patch_1")
    attn = attn_ref[...].reshape(FEAT, TOK).astype(F32).T.astype(BF16)
    output = dot(attn, weight_ref[...], NN)
    at = place * TOK + lax.broadcasted_iota(jnp.int32, (TOK, WIDTH), 0)
    error = jnp.where(at < len_ref[0], output - target_ref[0].astype(F32), 0.0)
    grad_out = (2.0 * error).T.astype(BF16)
    back = dot(weight_ref[...], grad_out, NN).astype(BF16)
    for h in range(HEADS):
        back_ref[h] = back[h * HD : (h + 1) * HD, :]
    out_ref[...] = grad_out
    loss = jnp.sum(error * error, axis=0, keepdims=True)
    loss_ref[...] = sum(loss[:, i * TOK : (i + 1) * TOK] for i in range(WIDTH // TOK))


def pair_kernel(attn_ref, grad_ref, loss_ref, pair_ref, half_ref):
    first = lax.axis_index("patch_1") == 0
    wide = attn_ref[...].reshape(FEAT, TOK).astype(F32)
    sides = []
    for side in (0, 1):
        pieces = [wide[p * ROWS : (p + 1) * ROWS] for p in range(side, PATCHES, 2)]
        sides.append(jnp.concatenate(pieces, axis=0))
    half_ref[...] = jnp.where(first, sides[0], sides[1]).astype(BF16)
    stats = jnp.concatenate([*high_low(loss_ref[...]), jnp.zeros((6, TOK), F32)], axis=0)
    pair_ref[0:WIDTH, :] = grad_ref[...]
    pair_ref[WIDTH : WIDTH + HALF, :] = jnp.where(first, sides[1], sides[0]).astype(BF16)
    pair_ref[WIDTH + HALF : PAIR, :] = stats.astype(BF16)


def weight_kernel(len_ref, mine_ref, got_ref, half_ref, out_ref, acc):
    left = jnp.concatenate([mine_ref[0:WIDTH, :], got_ref[0:WIDTH, :]], axis=1)
    right = jnp.concatenate([half_ref[...], got_ref[WIDTH : WIDTH + HALF, :]], axis=1)
    acc[:, 0:HALF] = dot(left, right, NT)
    upper = len_ref[0] // 256
    lower = len_ref[0] - upper * 256
    stats = mine_ref[WIDTH + HALF : PAIR, :].astype(F32) + got_ref[WIDTH + HALF : PAIR, :].astype(F32)
    loss_high, loss_low = high_low(stats[0:1] + stats[1:2])
    tail = jnp.concatenate(
        [
            jnp.full((1, TOK), upper.astype(F32)),
            jnp.full((1, TOK), lower.astype(F32)),
            loss_high,
            loss_low,
            jnp.zeros((PAD - STAT - 4, TOK), F32),
        ],
        axis=0,
    )
    part = COLS // 4
    for d in range(SAMPLES):
        at = d * COLS
        rest = [acc[at + i * part : at + (i + 1) * part, 2 * TOK : HALF] for i in range(4)]
        block = [
            acc[at : at + COLS, 0:TOK],
            acc[at : at + COLS, TOK : 2 * TOK],
            jnp.concatenate(rest, axis=1),
            tail,
        ]
        out_ref[d] = jnp.concatenate(block, axis=0).astype(BF16)


def backward_kernel(
    own_ref,
    other_ref,
    attn_ref,
    back_ref,
    probs_ref,
    inv_ref,
    query_out,
    own_out,
    other_out,
    value_sc,
    key_sc,
    key_acc,
    value_acc,
    probs_sc,
    sems,
):
    blocks = SEQ // 2 // QB
    copies = [pltpu.make_async_copy(probs_ref.at[b], probs_sc.at[b], sems.at[b]) for b in range(blocks)]
    for copy in copies:
        copy.start()
    for side, ref in enumerate((own_ref, other_ref)):
        for c in range(CHIPS):
            at = (side * CHIPS + c) * TOK
            value_sc[at : at + TOK, :] = ref[c, 2 * HD : 3 * HD, :].astype(F32).T.astype(BF16)
            key_sc[:, at : at + TOK] = ref[c, HD : 2 * HD, :]
    for b in range(SEQ // 2 // QB):
        pair = QB // TOK
        chips = range(b * pair, (b + 1) * pair)
        query = jnp.concatenate([own_ref[c, 0:HD, :] for c in chips], axis=1)
        attn = jnp.concatenate([attn_ref[c] for c in chips], axis=1)
        back = jnp.concatenate([back_ref[c] for c in chips], axis=1)
        back = (back.astype(F32) * inv_ref[b : b + 1, :]).astype(BF16)
        delta = jnp.sum(back.astype(F32) * attn.astype(F32), axis=0, keepdims=True)
        copies[b].wait()
        probs = probs_sc[b]
        dprobs = dot(value_sc[...], back, NN)
        dscores = (probs.astype(F32) * (dprobs - delta)).astype(BF16)
        query_grad = dot(key_sc[...], dscores, NN).astype(BF16)
        for i, c in enumerate(chips):
            query_out[c] = query_grad[:, i * TOK : (i + 1) * TOK]
        key_part = dot(query, dscores, NT)
        value_part = dot(back, probs, NT)
        if b == 0:
            key_acc[...] = key_part
            value_acc[...] = value_part
        else:
            key_acc[...] += key_part
            value_acc[...] += value_part
    for side, ref in enumerate((own_out, other_out)):
        for c in range(CHIPS):
            at = (side * CHIPS + c) * TOK
            ref[c, 0:HD, :] = key_acc[:, at : at + TOK].astype(BF16)
            ref[c, HD : 2 * HD, :] = value_acc[:, at : at + TOK].astype(BF16)


def join_kernel(query_ref, own_ref, other_ref, out_ref):
    out_ref[:, 0:HD, :] = query_ref[...]
    out_ref[:, HD : 3 * HD, :] = (own_ref[...].astype(F32) + other_ref[...].astype(F32)).astype(BF16)


def reduce_kernel(part_ref, join_ref, out_ref, stat_ref, last_sc, sem):
    del join_ref
    total = part_ref[0].astype(F32)
    for d in range(1, SAMPLES):
        total = total + part_ref[d].astype(F32)
    count = 256.0 * total[STAT : STAT + 1] + total[STAT + 1 : STAT + 2]
    stat_ref[...] = jnp.broadcast_to(count, (8, TOK))
    loss = total[STAT + 2 : STAT + 3] + total[STAT + 3 : STAT + 4]
    tail = jnp.concatenate([*high_low(loss), jnp.zeros((2, TOK), F32)], axis=0)
    rest = total[2 * COLS : STAT]
    width = HALF - 2 * TOK
    rest = jnp.concatenate([rest[:, i * width : (i + 1) * width] for i in range(4)], axis=0)
    rest = jnp.concatenate([rest, jnp.zeros((COLS, TOK - width), F32)], axis=1)
    block = jnp.concatenate([total[0:COLS], total[COLS : 2 * COLS], rest], axis=1)
    turned = jnp.concatenate([block, jnp.zeros((TOK - COLS, 3 * TOK), F32)], axis=0).T
    for c in range(CHIPS):
        block = jnp.concatenate([turned[c * ROWS : (c + 1) * ROWS, :], tail], axis=0)
        last_sc[c] = block.astype(BF16)
    copy = pltpu.make_async_copy(last_sc, out_ref.at[:, 3 * HD : 3 * HD + LAST, :], sem)
    copy.start()
    copy.wait()


def unpack_kernel(rows_ref, stat_ref, query_ref, key_ref, value_ref, weight_ref, loss_ref):
    count = stat_ref[0:1, :]
    ratio = float(SAMPLES * SEQ) / count
    for at, (ref, factor) in enumerate(((query_ref, SCALE), (key_ref, SCALE), (value_ref, 1.0))):
        for h in range(HEADS):
            rows = rows_ref[h, at * HD : (at + 1) * HD, :].astype(F32)
            ref[0, h * HD : (h + 1) * HD, :] = rows * (ratio * factor)
    total = sum(rows_ref[c, 3 * HD : 3 * HD + LAST, :].astype(F32) for c in range(CHIPS))
    weight_ref[...] = (total[0:ROWS, :] * (ratio / SEQ))[:, 0:COLS]
    loss = jnp.sum(total[ROWS : ROWS + 1, :] + total[ROWS + 1 : ROWS + 2, :], axis=1, keepdims=True)
    loss_ref[...] = loss / (count[:, 0:1] * WIDTH)


def in_hbm(value):
    return pltpu.with_memory_space_constraint(value, pltpu.HBM)


def exchange(value, axis):
    return lax.all_to_all(value, axis, 0, 0, tiled=True)


def swap(value):
    return lax.ppermute(value, "patch_1", [(0, 1), (1, 0)])


def shape(dims, dtype):
    return jax.ShapeDtypeStruct(dims, dtype)


def local(query_rows, key_rows, value_rows, out_weight, target, lengths, segments):
    buffer = shape((CHIPS, BUF, TOK), BF16)
    heads = shape((CHIPS, HD, TOK), BF16)
    turned = [
        in_hbm(jnp.swapaxes(rows, 1, 2).reshape(HEADS, HD, TOK))
        for rows in (query_rows, key_rows, value_rows)
    ]
    packed = call(
        pack_kernel,
        buffer,
        [HB] * 4,
        10**6,
        10**6,
        [pltpu.VMEM((1, TOK), jnp.int32), pltpu.SemaphoreType.DMA((4,))],
        2,
    )(*turned, in_hbm(segments))
    own = exchange(packed, "patch_0")
    other = swap(own)
    blocks = SEQ // 2 // QB
    attn, probs, inv = call(
        forward_kernel,
        (heads, pltpu.HBM((blocks, SEQ, QB), BF16), shape((blocks, QB), F32)),
        [SM, VM, VM],
        4 * HD * SEQ * SEQ // 2,
        6 * 10**6,
        [
            pltpu.VMEM((SEQ, HD), BF16),
            pltpu.VMEM((SEQ, TOK), F32),
            pltpu.VMEM((HD, SEQ), BF16),
            pltpu.VMEM((blocks, SEQ, QB), BF16),
            pltpu.SemaphoreType.DMA((blocks,)),
        ],
        24,
        (VM, HB, VM),
    )(lengths, own, other)
    attn_rows = exchange(attn, "patch_0")
    back, grad_out, loss_part = call(
        project_kernel,
        (heads, shape((WIDTH, TOK), BF16), shape((1, TOK), F32)),
        [SM, VM, VM, VM],
        4 * TOK * FEAT * WIDTH,
        3 * 10**6,
    )(lengths, attn_rows, out_weight, target)
    back_heads = exchange(back, "patch_0")
    mine, half = call(
        pair_kernel, (shape((PAIR, TOK), BF16), shape((HALF, TOK), BF16)), [VM] * 3, 10**6, 10**6
    )(attn_rows, grad_out, loss_part)
    got_pair = swap(mine)
    weight_part = call(
        weight_kernel,
        shape((SAMPLES, PAD, TOK), BF16),
        [SM, VM, VM, VM],
        2 * TOK * FEAT * WIDTH,
        3 * 10**6,
        [pltpu.VMEM((WIDTH, 3 * TOK), F32)],
    )(lengths, mine, got_pair, half)
    weight_parts = exchange(weight_part, DP)
    pair = shape((CHIPS, 2 * HD, TOK), BF16)
    query_grad, own_grad, other_grad = call(
        backward_kernel,
        (heads, pair, pair),
        [VM, VM, VM, VM, HB, VM],
        8 * HD * SEQ * SEQ // 2,
        6 * 10**6,
        [
            pltpu.VMEM((SEQ, HD), BF16),
            pltpu.VMEM((HD, SEQ), BF16),
            pltpu.VMEM((HD, SEQ), F32),
            pltpu.VMEM((HD, SEQ), F32),
            pltpu.VMEM((blocks, SEQ, QB), BF16),
            pltpu.SemaphoreType.DMA((blocks,)),
        ],
        24,
    )(own, other, attn, back_heads, in_hbm(probs), inv)
    got = swap(other_grad)
    both = shape((CHIPS, 3 * HD + LAST, TOK), BF16)
    joined = call(join_kernel, both, [VM] * 3, 10**6, 10**6)(query_grad, own_grad, got)
    joined, stats = call(
        reduce_kernel,
        (both, shape((8, TOK), F32)),
        [VM, ANY],
        10**6,
        10**6,
        [pltpu.VMEM((CHIPS, LAST, TOK), BF16), pltpu.SemaphoreType.DMA],
        outs=(ANY, VM),
        aliases={1: 0},
    )(weight_parts, joined)
    grads = exchange(joined, "patch_0")
    rows = shape((1, FEAT, TOK), F32)
    query_out, key_out, value_out, weight_grad, loss = call(
        unpack_kernel,
        (rows, rows, rows, shape((ROWS, COLS), F32), shape((1, 1), F32)),
        [VM, VM],
        10**6,
        10**6,
    )(grads, stats)
    grads_out = (jnp.swapaxes(rows, 1, 2) for rows in (query_out, key_out, value_out))
    return *grads_out, weight_grad, loss[0, 0]


def solution(mesh):
    torus = Mesh(mesh.devices.reshape(4, 8, 8, 2), ("dp_0", "dp_1", "patch_0", "patch_1"))
    return jax.shard_map(
        local,
        mesh=torus,
        in_specs=(
            P(DP, PATCH, None),
            P(DP, PATCH, None),
            P(DP, PATCH, None),
            P(),
            P(DP, PATCH, None),
            P(DP),
            P(DP, PATCH),
        ),
        out_specs=(P(DP, PATCH, None), P(DP, PATCH, None), P(DP, PATCH, None), P(PATCH, DP), P()),
        check_vma=False,
    )
```

```python
import math

import jax
import jax.numpy as jnp
from jax import lax
from jax.experimental import pallas as pl
from jax.experimental.pallas import tpu as pltpu
from jax.sharding import Mesh
from jax.sharding import PartitionSpec as P


WIDTH = 1152
HEADS = 8
HD = 72
TOK = 128
FEAT = 576
SEQ = 2048
SAMPLES = 32
CHIPS = 8
PATCHES = 16
COLS = WIDTH // SAMPLES
ROWS = FEAT // PATCHES
HALF = FEAT // 2
STAT = COLS * HALF // TOK
PAD = 88
THIRD = ROWS // 3
LAST = 16
DEPTH = 8
PAIR = WIDTH + HALF + 8
BUF = 3 * HD + 8
QB = 256
KEYS = 256
NEAR = 1
FAR = SEQ // 2 // QB - NEAR
NEG_LARGE = -1e30
SCALE = 1.0 / math.sqrt(HD)
EXP2_SCALE = SCALE * math.log2(math.e)
PATCH = ("patch_0", "patch_1")
DP = ("dp_0", "dp_1")
F32 = jnp.float32
BF16 = jnp.bfloat16

VM = pl.BlockSpec(memory_space=pltpu.VMEM)
SM = pl.BlockSpec(memory_space=pltpu.SMEM)
HB = pl.BlockSpec(memory_space=pltpu.HBM)
ANY = pl.BlockSpec(memory_space=pl.ANY)


def call(kernel, out_shape, in_specs, flops, nbytes, scratch=(), limit=16, outs=None, aliases=None):
    return pl.pallas_call(
        kernel,
        out_shape=out_shape,
        in_specs=in_specs,
        out_specs=outs if outs is not None else jax.tree.map(lambda _: VM, out_shape),
        scratch_shapes=list(scratch),
        input_output_aliases=aliases or {},
        cost_estimate=pl.CostEstimate(flops=flops, bytes_accessed=nbytes, transcendentals=0),
        compiler_params=pltpu.CompilerParams(vmem_limit_bytes=limit * 1024 * 1024),
    )


def dot(a, b, dims):
    return lax.dot_general(a, b, (dims, ((), ())), preferred_element_type=F32)


NN = ((1,), (0,))
NT = ((1,), (1,))


def pack_kernel(q_ref, k_ref, v_ref, seg_ref, out_ref, seg_sc, sems):
    copies = [
        pltpu.make_async_copy(ref, out_ref.at[:, at * HD : (at + 1) * HD, :], sems.at[at])
        for at, ref in enumerate((q_ref, k_ref, v_ref))
    ]
    copies.append(pltpu.make_async_copy(seg_ref, seg_sc, sems.at[3]))
    for copy in copies:
        copy.start()
    copies[3].wait()
    seg = jnp.broadcast_to(seg_sc[...].astype(F32), (8, TOK)).astype(BF16)
    for h in range(HEADS):
        out_ref[h, 3 * HD : BUF, :] = seg
    for copy in copies[:3]:
        copy.wait()


def group_rows(ref, chip, core, length):
    seg = ref[chip, 3 * HD : BUF, :].astype(F32)[0:1]
    at = (2 * chip + core) * TOK + lax.broadcasted_iota(jnp.int32, (1, TOK), 1)
    return jnp.where(at < length, seg, -1.0)


def forward_kernel(
    len_ref, own_ref, other_ref, attn_ref, near_ref, far_ref, inv_ref, key_sc, group_sc, value_sc, far_sc, sems, *score_refs
):
    core = lax.axis_index("patch_1")
    length = len_ref[0]
    own_groups = []
    copies = [pltpu.make_async_copy(far_sc.at[i], far_ref.at[i], sems.at[i]) for i in range(FAR)]
    for side, ref in enumerate((own_ref, other_ref)):
        for c in range(CHIPS):
            at = (side * CHIPS + c) * TOK
            key_sc[at : at + TOK, :] = ref[c, HD : 2 * HD, :].astype(F32).T.astype(BF16)
            value_sc[:, at : at + TOK] = ref[c, 2 * HD : 3 * HD, :]
            group = group_rows(ref, c, core if side == 0 else 1 - core, length)
            if side == 0:
                own_groups.append(group)
            group_sc[at : at + TOK, :] = jnp.broadcast_to(group, (TOK, TOK)).T
    order = (*range(NEAR, NEAR + FAR), *range(NEAR))
    pair = QB // TOK
    held = None
    for step in range(len(order) + 1):
        scores = score_refs[step % 2]
        if step < len(order):
            chips = range(order[step] * pair, (order[step] + 1) * pair)
            query = jnp.concatenate([own_ref[c, 0:HD, :] for c in chips], axis=1)
            group = jnp.concatenate([own_groups[c] for c in chips], axis=1)
            top = jnp.full((8, QB), NEG_LARGE, F32)
        if held is not None:
            b, held_scores, held_top = held
            weights_ref = near_ref.at[b] if b < NEAR else far_sc.at[b - NEAR]
            denom = jnp.zeros((8, QB), F32)
            accum = jnp.zeros((HD, QB), F32)
        for j in range(SEQ // KEYS):
            rows = slice(j * KEYS, (j + 1) * KEYS)
            if step < len(order):
                key_group = jnp.concatenate([group_sc[rows, :]] * pair, axis=1)
                masked = jnp.where(key_group == group, dot(key_sc[rows, :], query, NN), NEG_LARGE)
                scores[rows, :] = masked
                top = jnp.maximum(top, jnp.max(masked.reshape(KEYS // 8, 8, QB), axis=0))
            if held is not None:
                probs = jnp.exp2((held_scores[rows, :] - held_top) * EXP2_SCALE)
                denom = denom + jnp.sum(probs.reshape(KEYS // 8, 8, QB), axis=0)
                weights = probs.astype(BF16)
                weights_ref[rows, :] = weights
                accum = accum + dot(value_sc[:, rows], weights, NN)
        if held is not None:
            if b >= NEAR:
                copies[b - NEAR].start()
            inv = 1.0 / jnp.sum(denom, axis=0, keepdims=True)
            attn = (accum * inv).astype(BF16)
            inv_ref[b : b + 1, :] = inv
            for i in range(pair):
                attn_ref[b * pair + i] = attn[:, i * TOK : (i + 1) * TOK]
        if step < len(order):
            held = (order[step], scores, jnp.max(top, axis=0, keepdims=True))
    for copy in copies:
        copy.wait()


def high_low(value):
    high = value.astype(BF16).astype(F32)
    return high, value - high


def project_kernel(len_ref, attn_ref, weight_ref, target_ref, back_ref, out_ref, loss_ref):
    place = 2 * lax.axis_index("patch_0") + lax.axis_index("patch_1")
    attn = attn_ref[...].reshape(FEAT, TOK).astype(F32).T.astype(BF16)
    output = dot(attn, weight_ref[...], NN)
    at = place * TOK + lax.broadcasted_iota(jnp.int32, (TOK, WIDTH), 0)
    error = jnp.where(at < len_ref[0], output - target_ref[0].astype(F32), 0.0)
    grad_out = (2.0 * error).T.astype(BF16)
    back = dot(weight_ref[...], grad_out, NN).astype(BF16)
    for h in range(HEADS):
        back_ref[h] = back[h * HD : (h + 1) * HD, :]
    out_ref[...] = grad_out
    loss = jnp.sum(error * error, axis=0, keepdims=True)
    loss_ref[...] = sum(loss[:, i * TOK : (i + 1) * TOK] for i in range(WIDTH // TOK))


def pair_kernel(attn_ref, grad_ref, loss_ref, pair_ref, half_ref):
    first = lax.axis_index("patch_1") == 0
    wide = attn_ref[...].reshape(FEAT, TOK).astype(F32)
    sides = []
    for side in (0, 1):
        pieces = [wide[p * ROWS : (p + 1) * ROWS] for p in range(side, PATCHES, 2)]
        sides.append(jnp.concatenate(pieces, axis=0))
    half_ref[...] = jnp.where(first, sides[0], sides[1]).astype(BF16)
    stats = jnp.concatenate([*high_low(loss_ref[...]), jnp.zeros((6, TOK), F32)], axis=0)
    pair_ref[0:WIDTH, :] = grad_ref[...]
    pair_ref[WIDTH : WIDTH + HALF, :] = jnp.where(first, sides[1], sides[0]).astype(BF16)
    pair_ref[WIDTH + HALF : PAIR, :] = stats.astype(BF16)


def stat_rows(count, loss):
    upper = jnp.floor(count * (1.0 / 256.0))
    rows = [upper, count - 256.0 * upper, *high_low(loss), jnp.zeros((PAD - STAT - 4, TOK), F32)]
    return jnp.concatenate(rows, axis=0)


def stats_of(block):
    count = 256.0 * block[STAT : STAT + 1] + block[STAT + 1 : STAT + 2]
    return count, block[STAT + 2 : STAT + 3] + block[STAT + 3 : STAT + 4]


def weight_kernel(len_ref, mine_ref, got_ref, half_ref, out_ref, acc):
    left = jnp.concatenate([mine_ref[0:WIDTH, :], got_ref[0:WIDTH, :]], axis=1)
    right = jnp.concatenate([half_ref[...], got_ref[WIDTH : WIDTH + HALF, :]], axis=1)
    acc[:, 0:HALF] = dot(left, right, NT)
    stats = mine_ref[WIDTH + HALF : PAIR, :].astype(F32) + got_ref[WIDTH + HALF : PAIR, :].astype(F32)
    tail = stat_rows(jnp.full((1, TOK), len_ref[0].astype(F32)), stats[0:1] + stats[1:2])
    part = COLS // 4
    for d in range(SAMPLES):
        at = d * COLS
        rest = [acc[at + i * part : at + (i + 1) * part, 2 * TOK : HALF] for i in range(4)]
        block = [
            acc[at : at + COLS, 0:TOK],
            acc[at : at + COLS, TOK : 2 * TOK],
            jnp.concatenate(rest, axis=1),
            tail,
        ]
        out_ref[d // DEPTH, d % DEPTH] = jnp.concatenate(block, axis=0).astype(BF16)


def sum_kernel(part_ref, out_ref):
    total = part_ref[0].astype(F32)
    for x in range(1, SAMPLES // DEPTH):
        total = total + part_ref[x].astype(F32)
    out_ref[...] = total.astype(BF16)
    tail = stat_rows(*stats_of(total[0])).astype(BF16)
    for z in range(DEPTH):
        out_ref[z, STAT:PAD, :] = tail


def backward_kernel(
    own_ref,
    other_ref,
    attn_ref,
    back_ref,
    near_ref,
    far_ref,
    inv_ref,
    query_out,
    own_out,
    other_out,
    value_sc,
    key_sc,
    key_acc,
    value_acc,
    far_sc,
    sems,
):
    copies = [pltpu.make_async_copy(far_ref.at[i], far_sc.at[i], sems.at[i]) for i in range(FAR)]
    for copy in copies:
        copy.start()
    for side, ref in enumerate((own_ref, other_ref)):
        for c in range(CHIPS):
            at = (side * CHIPS + c) * TOK
            value_sc[at : at + TOK, :] = ref[c, 2 * HD : 3 * HD, :].astype(F32).T.astype(BF16)
            key_sc[:, at : at + TOK] = ref[c, HD : 2 * HD, :]
    for b in range(SEQ // 2 // QB):
        pair = QB // TOK
        chips = range(b * pair, (b + 1) * pair)
        query = jnp.concatenate([own_ref[c, 0:HD, :] for c in chips], axis=1)
        attn = jnp.concatenate([attn_ref[c] for c in chips], axis=1)
        back = jnp.concatenate([back_ref[c] for c in chips], axis=1)
        back = (back.astype(F32) * inv_ref[b : b + 1, :]).astype(BF16)
        delta = jnp.sum(back.astype(F32) * attn.astype(F32), axis=0, keepdims=True)
        if b == NEAR:
            for copy in copies:
                copy.wait()
        probs = near_ref[b] if b < NEAR else far_sc[b - NEAR]
        dprobs = dot(value_sc[...], back, NN)
        dscores = (probs.astype(F32) * (dprobs - delta)).astype(BF16)
        query_grad = dot(key_sc[...], dscores, NN).astype(BF16)
        for i, c in enumerate(chips):
            query_out[c] = query_grad[:, i * TOK : (i + 1) * TOK]
        key_part = dot(query, dscores, NT)
        value_part = dot(back, probs, NT)
        if b == 0:
            key_acc[...] = key_part
            value_acc[...] = value_part
        else:
            key_acc[...] += key_part
            value_acc[...] += value_part
    for side, ref in enumerate((own_out, other_out)):
        for c in range(CHIPS):
            at = (side * CHIPS + c) * TOK
            ref[c, 0:HD, :] = key_acc[:, at : at + TOK].astype(BF16)
            ref[c, HD : 2 * HD, :] = value_acc[:, at : at + TOK].astype(BF16)


def join_kernel(query_ref, own_ref, other_ref, out_ref):
    out_ref[:, 0:HD, :] = query_ref[...]
    out_ref[:, HD : 3 * HD, :] = (own_ref[...].astype(F32) + other_ref[...].astype(F32)).astype(BF16)


def reduce_kernel(part_ref, join_ref, out_ref, stat_ref, last_sc, sem):
    del join_ref
    total = part_ref[0].astype(F32)
    for d in range(1, DEPTH):
        total = total + part_ref[d].astype(F32)
    count, loss = stats_of(total)
    stat_ref[...] = jnp.broadcast_to(count, (8, TOK))
    rest = total[2 * COLS : STAT]
    width = HALF - 2 * TOK
    rest = jnp.concatenate([rest[:, i * width : (i + 1) * width] for i in range(4)], axis=0)
    rest = jnp.concatenate([rest, jnp.zeros((COLS, TOK - width), F32)], axis=1)
    block = jnp.concatenate([total[0:COLS], total[COLS : 2 * COLS], rest], axis=1)
    turned = jnp.concatenate([block, jnp.zeros((TOK - COLS, 3 * TOK), F32)], axis=0).T
    loss = jnp.concatenate([*high_low(loss), jnp.zeros((LAST - THIRD - 2, TOK), F32)], axis=0)
    for c in range(CHIPS):
        thirds = [turned[c * ROWS + i * THIRD : c * ROWS + (i + 1) * THIRD, 0:COLS] for i in range(3)]
        rows = jnp.concatenate([*thirds, jnp.zeros((THIRD, TOK - 3 * COLS), F32)], axis=1)
        last_sc[c] = jnp.concatenate([rows, loss], axis=0).astype(BF16)
    copy = pltpu.make_async_copy(last_sc, out_ref.at[:, 3 * HD : 3 * HD + LAST, :], sem)
    copy.start()
    copy.wait()


def unpack_kernel(rows_ref, stat_ref, query_ref, key_ref, value_ref, weight_ref, loss_ref):
    count = stat_ref[0:1, :]
    ratio = float(SAMPLES * SEQ) / count
    for at, (ref, factor) in enumerate(((query_ref, SCALE), (key_ref, SCALE), (value_ref, 1.0))):
        for h in range(HEADS):
            rows = rows_ref[h, at * HD : (at + 1) * HD, :].astype(F32)
            ref[0, h * HD : (h + 1) * HD, :] = rows * (ratio * factor)
    total = sum(rows_ref[c, 3 * HD : 3 * HD + LAST, :].astype(F32) for c in range(CHIPS))
    scaled = total * (ratio / SEQ)
    thirds = [scaled[0:THIRD, i * COLS : (i + 1) * COLS] for i in range(3)]
    weight_ref[...] = jnp.concatenate(thirds, axis=0)
    loss = jnp.sum(total[THIRD : THIRD + 1] + total[THIRD + 1 : THIRD + 2], axis=1, keepdims=True)
    loss_ref[...] = loss / (count[:, 0:1] * WIDTH)


def in_hbm(value):
    return pltpu.with_memory_space_constraint(value, pltpu.HBM)


def exchange(value, axis):
    return lax.all_to_all(value, axis, 0, 0, tiled=True)


def swap(value):
    return lax.ppermute(value, "patch_1", [(0, 1), (1, 0)])


def shape(dims, dtype):
    return jax.ShapeDtypeStruct(dims, dtype)


def local(query_rows, key_rows, value_rows, out_weight, target, lengths, segments):
    buffer = shape((CHIPS, BUF, TOK), BF16)
    heads = shape((CHIPS, HD, TOK), BF16)
    turned = [
        in_hbm(jnp.swapaxes(rows, 1, 2).reshape(HEADS, HD, TOK))
        for rows in (query_rows, key_rows, value_rows)
    ]
    packed = call(
        pack_kernel,
        buffer,
        [HB] * 4,
        10**6,
        10**6,
        [pltpu.VMEM((1, TOK), jnp.int32), pltpu.SemaphoreType.DMA((4,))],
        2,
    )(*turned, in_hbm(segments))
    own = exchange(packed, "patch_0")
    other = swap(own)
    blocks = SEQ // 2 // QB
    attn, near, far, inv = call(
        forward_kernel,
        (heads, shape((NEAR, SEQ, QB), BF16), pltpu.HBM((FAR, SEQ, QB), BF16), shape((blocks, QB), F32)),
        [SM, VM, VM],
        4 * HD * SEQ * SEQ // 2,
        6 * 10**6,
        [
            pltpu.VMEM((SEQ, HD), BF16),
            pltpu.VMEM((SEQ, TOK), F32),
            pltpu.VMEM((HD, SEQ), BF16),
            pltpu.VMEM((FAR, SEQ, QB), BF16),
            pltpu.SemaphoreType.DMA((FAR,)),
            pltpu.VMEM((SEQ, QB), F32),
            pltpu.VMEM((SEQ, QB), F32),
        ],
        24,
        (VM, VM, HB, VM),
    )(lengths, own, other)
    attn_rows = exchange(attn, "patch_0")
    back, grad_out, loss_part = call(
        project_kernel,
        (heads, shape((WIDTH, TOK), BF16), shape((1, TOK), F32)),
        [SM, VM, VM, VM],
        4 * TOK * FEAT * WIDTH,
        3 * 10**6,
    )(lengths, attn_rows, out_weight, target)
    back_heads = exchange(back, "patch_0")
    mine, half = call(
        pair_kernel, (shape((PAIR, TOK), BF16), shape((HALF, TOK), BF16)), [VM] * 3, 10**6, 10**6
    )(attn_rows, grad_out, loss_part)
    got_pair = swap(mine)
    weight_part = call(
        weight_kernel,
        shape((SAMPLES // DEPTH, DEPTH, PAD, TOK), BF16),
        [SM, VM, VM, VM],
        2 * TOK * FEAT * WIDTH,
        3 * 10**6,
        [pltpu.VMEM((WIDTH, 3 * TOK), F32)],
    )(lengths, mine, got_pair, half)
    weight_rows = exchange(weight_part, "dp_0")
    pair = shape((CHIPS, 2 * HD, TOK), BF16)
    query_grad, own_grad, other_grad = call(
        backward_kernel,
        (heads, pair, pair),
        [VM, VM, VM, VM, VM, HB, VM],
        8 * HD * SEQ * SEQ // 2,
        6 * 10**6,
        [
            pltpu.VMEM((SEQ, HD), BF16),
            pltpu.VMEM((HD, SEQ), BF16),
            pltpu.VMEM((HD, SEQ), F32),
            pltpu.VMEM((HD, SEQ), F32),
            pltpu.VMEM((FAR, SEQ, QB), BF16),
            pltpu.SemaphoreType.DMA((FAR,)),
        ],
        24,
    )(own, other, attn, back_heads, near, in_hbm(far), inv)
    weight_row = call(sum_kernel, shape((DEPTH, PAD, TOK), BF16), [VM], 10**6, 10**6)(weight_rows)
    weight_parts = exchange(weight_row, "dp_1")
    got = swap(other_grad)
    both = shape((CHIPS, 3 * HD + LAST, TOK), BF16)
    joined = call(join_kernel, both, [VM] * 3, 10**6, 10**6)(query_grad, own_grad, got)
    joined, stats = call(
        reduce_kernel,
        (both, shape((8, TOK), F32)),
        [VM, ANY],
        10**6,
        10**6,
        [pltpu.VMEM((CHIPS, LAST, TOK), BF16), pltpu.SemaphoreType.DMA],
        outs=(ANY, VM),
        aliases={1: 0},
    )(weight_parts, joined)
    grads = exchange(joined, "patch_0")
    rows = shape((1, FEAT, TOK), F32)
    query_out, key_out, value_out, weight_grad, loss = call(
        unpack_kernel,
        (rows, rows, rows, shape((ROWS, COLS), F32), shape((1, 1), F32)),
        [VM, VM],
        10**6,
        10**6,
    )(grads, stats)
    grads_out = (jnp.swapaxes(rows, 1, 2) for rows in (query_out, key_out, value_out))
    return *grads_out, weight_grad, loss[0, 0]


def solution(mesh):
    torus = Mesh(mesh.devices.reshape(4, 8, 8, 2), ("dp_0", "dp_1", "patch_0", "patch_1"))
    return jax.shard_map(
        local,
        mesh=torus,
        in_specs=(
            P(DP, PATCH, None),
            P(DP, PATCH, None),
            P(DP, PATCH, None),
            P(),
            P(DP, PATCH, None),
            P(DP),
            P(DP, PATCH),
        ),
        out_specs=(P(DP, PATCH, None), P(DP, PATCH, None), P(DP, PATCH, None), P(PATCH, DP), P()),
        check_vma=False,
    )
```

```python
import math

import jax
import jax.numpy as jnp
from jax import lax
from jax.experimental import pallas as pl
from jax.experimental.pallas import tpu as pltpu
from jax.sharding import Mesh
from jax.sharding import PartitionSpec as P


WIDTH = 1152
HEADS = 8
HD = 72
TOK = 128
FEAT = 576
SEQ = 2048
SAMPLES = 32
CHIPS = 8
PATCHES = 16
COLS = WIDTH // SAMPLES
ROWS = FEAT // PATCHES
HALF = FEAT // 2
STAT = COLS * HALF // TOK
PAD = 88
THIRD = ROWS // 3
LAST = 16
PAIR = WIDTH + HALF + 8
BUF = 3 * HD + 8
QB = 256
KEYS = 256
NEAR = 1
FAR = SEQ // 2 // QB - NEAR
NEG_LARGE = -1e30
SCALE = 1.0 / math.sqrt(HD)
EXP2_SCALE = SCALE * math.log2(math.e)
PATCH = ("patch_0", "patch_1")
DP = ("dp_0", "dp_1")
F32 = jnp.float32
BF16 = jnp.bfloat16

VM = pl.BlockSpec(memory_space=pltpu.VMEM)
SM = pl.BlockSpec(memory_space=pltpu.SMEM)
HB = pl.BlockSpec(memory_space=pltpu.HBM)
ANY = pl.BlockSpec(memory_space=pl.ANY)


def call(kernel, out_shape, in_specs, flops, nbytes, scratch=(), limit=16, outs=None, aliases=None):
    return pl.pallas_call(
        kernel,
        out_shape=out_shape,
        in_specs=in_specs,
        out_specs=outs if outs is not None else jax.tree.map(lambda _: VM, out_shape),
        scratch_shapes=list(scratch),
        input_output_aliases=aliases or {},
        cost_estimate=pl.CostEstimate(flops=flops, bytes_accessed=nbytes, transcendentals=0),
        compiler_params=pltpu.CompilerParams(vmem_limit_bytes=limit * 1024 * 1024),
    )


def dot(a, b, dims):
    return lax.dot_general(a, b, (dims, ((), ())), preferred_element_type=F32)


NN = ((1,), (0,))
NT = ((1,), (1,))


def pack_kernel(q_ref, k_ref, v_ref, seg_ref, out_ref, seg_sc, sems):
    copies = [
        pltpu.make_async_copy(ref, out_ref.at[:, at * HD : (at + 1) * HD, :], sems.at[at])
        for at, ref in enumerate((q_ref, k_ref, v_ref))
    ]
    copies.append(pltpu.make_async_copy(seg_ref, seg_sc, sems.at[3]))
    for copy in copies:
        copy.start()
    copies[3].wait()
    seg = jnp.broadcast_to(seg_sc[...].astype(F32), (8, TOK)).astype(BF16)
    for h in range(HEADS):
        out_ref[h, 3 * HD : BUF, :] = seg
    for copy in copies[:3]:
        copy.wait()


def group_rows(ref, chip, core, length):
    seg = ref[chip, 3 * HD : BUF, :].astype(F32)[0:1]
    at = (2 * chip + core) * TOK + lax.broadcasted_iota(jnp.int32, (1, TOK), 1)
    return jnp.where(at < length, seg, -1.0)


def forward_kernel(
    len_ref, own_ref, other_ref, attn_ref, near_ref, far_ref, inv_ref, key_sc, group_sc, value_sc, far_sc, sems, *score_refs
):
    core = lax.axis_index("patch_1")
    length = len_ref[0]
    own_groups = []
    copies = [pltpu.make_async_copy(far_sc.at[i], far_ref.at[i], sems.at[i]) for i in range(FAR)]
    for side, ref in enumerate((own_ref, other_ref)):
        for c in range(CHIPS):
            at = (side * CHIPS + c) * TOK
            key_sc[at : at + TOK, :] = ref[c, HD : 2 * HD, :].astype(F32).T.astype(BF16)
            value_sc[:, at : at + TOK] = ref[c, 2 * HD : 3 * HD, :]
            group = group_rows(ref, c, core if side == 0 else 1 - core, length)
            if side == 0:
                own_groups.append(group)
            group_sc[at : at + TOK, :] = jnp.broadcast_to(group, (TOK, TOK)).T
    order = (*range(NEAR, NEAR + FAR), *range(NEAR))
    pair = QB // TOK
    held = None
    for step in range(len(order) + 1):
        scores = score_refs[step % 2]
        if step < len(order):
            chips = range(order[step] * pair, (order[step] + 1) * pair)
            query = jnp.concatenate([own_ref[c, 0:HD, :] for c in chips], axis=1)
            group = jnp.concatenate([own_groups[c] for c in chips], axis=1)
            top = jnp.full((8, QB), NEG_LARGE, F32)
        if held is not None:
            b, held_scores, held_top = held
            weights_ref = near_ref.at[b] if b < NEAR else far_sc.at[b - NEAR]
            denom = jnp.zeros((8, QB), F32)
            accum = jnp.zeros((HD, QB), F32)
        for j in range(SEQ // KEYS):
            rows = slice(j * KEYS, (j + 1) * KEYS)
            if step < len(order):
                key_group = jnp.concatenate([group_sc[rows, :]] * pair, axis=1)
                masked = jnp.where(key_group == group, dot(key_sc[rows, :], query, NN), NEG_LARGE)
                scores[rows, :] = masked
                top = jnp.maximum(top, jnp.max(masked.reshape(KEYS // 8, 8, QB), axis=0))
            if held is not None:
                probs = jnp.exp2((held_scores[rows, :] - held_top) * EXP2_SCALE)
                denom = denom + jnp.sum(probs.reshape(KEYS // 8, 8, QB), axis=0)
                weights = probs.astype(BF16)
                weights_ref[rows, :] = weights
                accum = accum + dot(value_sc[:, rows], weights, NN)
        if held is not None:
            if b >= NEAR:
                copies[b - NEAR].start()
            inv = 1.0 / jnp.sum(denom, axis=0, keepdims=True)
            attn = (accum * inv).astype(BF16)
            inv_ref[b : b + 1, :] = inv
            for i in range(pair):
                attn_ref[b * pair + i] = attn[:, i * TOK : (i + 1) * TOK]
        if step < len(order):
            held = (order[step], scores, jnp.max(top, axis=0, keepdims=True))
    for copy in copies:
        copy.wait()


def high_low(value):
    high = value.astype(BF16).astype(F32)
    return high, value - high


def project_kernel(len_ref, attn_ref, weight_ref, target_ref, back_ref, out_ref, loss_ref):
    place = 2 * lax.axis_index("patch_0") + lax.axis_index("patch_1")
    attn = attn_ref[...].reshape(FEAT, TOK).astype(F32).T.astype(BF16)
    output = dot(attn, weight_ref[...], NN)
    at = place * TOK + lax.broadcasted_iota(jnp.int32, (TOK, WIDTH), 0)
    error = jnp.where(at < len_ref[0], output - target_ref[0].astype(F32), 0.0)
    grad_out = (2.0 * error).T.astype(BF16)
    back = dot(weight_ref[...], grad_out, NN).astype(BF16)
    for h in range(HEADS):
        back_ref[h] = back[h * HD : (h + 1) * HD, :]
    out_ref[...] = grad_out
    loss = jnp.sum(error * error, axis=0, keepdims=True)
    loss_ref[...] = sum(loss[:, i * TOK : (i + 1) * TOK] for i in range(WIDTH // TOK))


def pair_kernel(attn_ref, grad_ref, loss_ref, pair_ref, half_ref):
    first = lax.axis_index("patch_1") == 0
    wide = attn_ref[...].reshape(FEAT, TOK).astype(F32)
    sides = []
    for side in (0, 1):
        pieces = [wide[p * ROWS : (p + 1) * ROWS] for p in range(side, PATCHES, 2)]
        sides.append(jnp.concatenate(pieces, axis=0))
    half_ref[...] = jnp.where(first, sides[0], sides[1]).astype(BF16)
    stats = jnp.concatenate([*high_low(loss_ref[...]), jnp.zeros((6, TOK), F32)], axis=0)
    pair_ref[0:WIDTH, :] = grad_ref[...]
    pair_ref[WIDTH : WIDTH + HALF, :] = jnp.where(first, sides[1], sides[0]).astype(BF16)
    pair_ref[WIDTH + HALF : PAIR, :] = stats.astype(BF16)


def stat_rows(count, loss):
    upper = jnp.floor(count * (1.0 / 256.0))
    rows = [upper, count - 256.0 * upper, *high_low(loss), jnp.zeros((PAD - STAT - 4, TOK), F32)]
    return jnp.concatenate(rows, axis=0)


def stats_of(block):
    count = 256.0 * block[STAT : STAT + 1] + block[STAT + 1 : STAT + 2]
    return count, block[STAT + 2 : STAT + 3] + block[STAT + 3 : STAT + 4]


def weight_kernel(len_ref, mine_ref, got_ref, half_ref, out_ref, acc):
    left = jnp.concatenate([mine_ref[0:WIDTH, :], got_ref[0:WIDTH, :]], axis=1)
    right = jnp.concatenate([half_ref[...], got_ref[WIDTH : WIDTH + HALF, :]], axis=1)
    acc[:, 0:HALF] = dot(left, right, NT)
    stats = mine_ref[WIDTH + HALF : PAIR, :].astype(F32) + got_ref[WIDTH + HALF : PAIR, :].astype(F32)
    tail = stat_rows(jnp.full((1, TOK), len_ref[0].astype(F32)), stats[0:1] + stats[1:2])
    part = COLS // 4
    for d in range(SAMPLES):
        at = d * COLS
        rest = [acc[at + i * part : at + (i + 1) * part, 2 * TOK : HALF] for i in range(4)]
        block = [
            acc[at : at + COLS, 0:TOK],
            acc[at : at + COLS, TOK : 2 * TOK],
            jnp.concatenate(rest, axis=1),
            tail,
        ]
        out_ref[d] = jnp.concatenate(block, axis=0).astype(BF16)


def backward_kernel(
    own_ref,
    other_ref,
    attn_ref,
    back_ref,
    near_ref,
    far_ref,
    inv_ref,
    query_out,
    own_out,
    other_out,
    value_sc,
    key_sc,
    key_acc,
    value_acc,
    far_sc,
    sems,
):
    copies = [pltpu.make_async_copy(far_ref.at[i], far_sc.at[i], sems.at[i]) for i in range(FAR)]
    for copy in copies:
        copy.start()
    for side, ref in enumerate((own_ref, other_ref)):
        for c in range(CHIPS):
            at = (side * CHIPS + c) * TOK
            value_sc[at : at + TOK, :] = ref[c, 2 * HD : 3 * HD, :].astype(F32).T.astype(BF16)
            key_sc[:, at : at + TOK] = ref[c, HD : 2 * HD, :]
    for b in range(SEQ // 2 // QB):
        pair = QB // TOK
        chips = range(b * pair, (b + 1) * pair)
        query = jnp.concatenate([own_ref[c, 0:HD, :] for c in chips], axis=1)
        attn = jnp.concatenate([attn_ref[c] for c in chips], axis=1)
        back = jnp.concatenate([back_ref[c] for c in chips], axis=1)
        back = (back.astype(F32) * inv_ref[b : b + 1, :]).astype(BF16)
        delta = jnp.sum(back.astype(F32) * attn.astype(F32), axis=0, keepdims=True)
        if b == NEAR:
            for copy in copies:
                copy.wait()
        probs = near_ref[b] if b < NEAR else far_sc[b - NEAR]
        dprobs = dot(value_sc[...], back, NN)
        dscores = (probs.astype(F32) * (dprobs - delta)).astype(BF16)
        query_grad = dot(key_sc[...], dscores, NN).astype(BF16)
        for i, c in enumerate(chips):
            query_out[c] = query_grad[:, i * TOK : (i + 1) * TOK]
        key_part = dot(query, dscores, NT)
        value_part = dot(back, probs, NT)
        if b == 0:
            key_acc[...] = key_part
            value_acc[...] = value_part
        else:
            key_acc[...] += key_part
            value_acc[...] += value_part
    for side, ref in enumerate((own_out, other_out)):
        for c in range(CHIPS):
            at = (side * CHIPS + c) * TOK
            ref[c, 0:HD, :] = key_acc[:, at : at + TOK].astype(BF16)
            ref[c, HD : 2 * HD, :] = value_acc[:, at : at + TOK].astype(BF16)


def join_kernel(query_ref, own_ref, other_ref, out_ref):
    out_ref[:, 0:HD, :] = query_ref[...]
    out_ref[:, HD : 3 * HD, :] = (own_ref[...].astype(F32) + other_ref[...].astype(F32)).astype(BF16)


def reduce_kernel(part_ref, join_ref, out_ref, stat_ref, last_sc, sem):
    del join_ref
    total = part_ref[0].astype(F32)
    for d in range(1, SAMPLES):
        total = total + part_ref[d].astype(F32)
    count, loss = stats_of(total)
    stat_ref[...] = jnp.broadcast_to(count, (8, TOK))
    rest = total[2 * COLS : STAT]
    width = HALF - 2 * TOK
    rest = jnp.concatenate([rest[:, i * width : (i + 1) * width] for i in range(4)], axis=0)
    rest = jnp.concatenate([rest, jnp.zeros((COLS, TOK - width), F32)], axis=1)
    block = jnp.concatenate([total[0:COLS], total[COLS : 2 * COLS], rest], axis=1)
    turned = jnp.concatenate([block, jnp.zeros((TOK - COLS, 3 * TOK), F32)], axis=0).T
    loss = jnp.concatenate([*high_low(loss), jnp.zeros((LAST - THIRD - 2, TOK), F32)], axis=0)
    for c in range(CHIPS):
        thirds = [turned[c * ROWS + i * THIRD : c * ROWS + (i + 1) * THIRD, 0:COLS] for i in range(3)]
        rows = jnp.concatenate([*thirds, jnp.zeros((THIRD, TOK - 3 * COLS), F32)], axis=1)
        last_sc[c] = jnp.concatenate([rows, loss], axis=0).astype(BF16)
    copy = pltpu.make_async_copy(last_sc, out_ref.at[:, 3 * HD : 3 * HD + LAST, :], sem)
    copy.start()
    copy.wait()


def unpack_kernel(rows_ref, stat_ref, query_ref, key_ref, value_ref, weight_ref, loss_ref):
    count = stat_ref[0:1, :]
    ratio = float(SAMPLES * SEQ) / count
    for at, (ref, factor) in enumerate(((query_ref, SCALE), (key_ref, SCALE), (value_ref, 1.0))):
        for h in range(HEADS):
            rows = rows_ref[h, at * HD : (at + 1) * HD, :].astype(F32)
            ref[0, h * HD : (h + 1) * HD, :] = rows * (ratio * factor)
    total = sum(rows_ref[c, 3 * HD : 3 * HD + LAST, :].astype(F32) for c in range(CHIPS))
    scaled = total * (ratio / SEQ)
    thirds = [scaled[0:THIRD, i * COLS : (i + 1) * COLS] for i in range(3)]
    weight_ref[...] = jnp.concatenate(thirds, axis=0)
    loss = jnp.sum(total[THIRD : THIRD + 1] + total[THIRD + 1 : THIRD + 2], axis=1, keepdims=True)
    loss_ref[...] = loss / (count[:, 0:1] * WIDTH)


def in_hbm(value):
    return pltpu.with_memory_space_constraint(value, pltpu.HBM)


def exchange(value, axis):
    return lax.all_to_all(value, axis, 0, 0, tiled=True)


def swap(value):
    return lax.ppermute(value, "patch_1", [(0, 1), (1, 0)])


def shape(dims, dtype):
    return jax.ShapeDtypeStruct(dims, dtype)


def local(query_rows, key_rows, value_rows, out_weight, target, lengths, segments):
    buffer = shape((CHIPS, BUF, TOK), BF16)
    heads = shape((CHIPS, HD, TOK), BF16)
    turned = [
        in_hbm(jnp.swapaxes(rows, 1, 2).reshape(HEADS, HD, TOK))
        for rows in (query_rows, key_rows, value_rows)
    ]
    packed = call(
        pack_kernel,
        buffer,
        [HB] * 4,
        10**6,
        10**6,
        [pltpu.VMEM((1, TOK), jnp.int32), pltpu.SemaphoreType.DMA((4,))],
        2,
    )(*turned, in_hbm(segments))
    own = exchange(packed, "patch_0")
    other = swap(own)
    blocks = SEQ // 2 // QB
    attn, near, far, inv = call(
        forward_kernel,
        (heads, shape((NEAR, SEQ, QB), BF16), pltpu.HBM((FAR, SEQ, QB), BF16), shape((blocks, QB), F32)),
        [SM, VM, VM],
        4 * HD * SEQ * SEQ // 2,
        6 * 10**6,
        [
            pltpu.VMEM((SEQ, HD), BF16),
            pltpu.VMEM((SEQ, TOK), F32),
            pltpu.VMEM((HD, SEQ), BF16),
            pltpu.VMEM((FAR, SEQ, QB), BF16),
            pltpu.SemaphoreType.DMA((FAR,)),
            pltpu.VMEM((SEQ, QB), F32),
            pltpu.VMEM((SEQ, QB), F32),
        ],
        24,
        (VM, VM, HB, VM),
    )(lengths, own, other)
    attn_rows = exchange(attn, "patch_0")
    back, grad_out, loss_part = call(
        project_kernel,
        (heads, shape((WIDTH, TOK), BF16), shape((1, TOK), F32)),
        [SM, VM, VM, VM],
        4 * TOK * FEAT * WIDTH,
        3 * 10**6,
    )(lengths, attn_rows, out_weight, target)
    back_heads = exchange(back, "patch_0")
    mine, half = call(
        pair_kernel, (shape((PAIR, TOK), BF16), shape((HALF, TOK), BF16)), [VM] * 3, 10**6, 10**6
    )(attn_rows, grad_out, loss_part)
    got_pair = swap(mine)
    weight_part = call(
        weight_kernel,
        shape((SAMPLES, PAD, TOK), BF16),
        [SM, VM, VM, VM],
        2 * TOK * FEAT * WIDTH,
        3 * 10**6,
        [pltpu.VMEM((WIDTH, 3 * TOK), F32)],
    )(lengths, mine, got_pair, half)
    weight_parts = exchange(weight_part, DP)
    pair = shape((CHIPS, 2 * HD, TOK), BF16)
    query_grad, own_grad, other_grad = call(
        backward_kernel,
        (heads, pair, pair),
        [VM, VM, VM, VM, VM, HB, VM],
        8 * HD * SEQ * SEQ // 2,
        6 * 10**6,
        [
            pltpu.VMEM((SEQ, HD), BF16),
            pltpu.VMEM((HD, SEQ), BF16),
            pltpu.VMEM((HD, SEQ), F32),
            pltpu.VMEM((HD, SEQ), F32),
            pltpu.VMEM((FAR, SEQ, QB), BF16),
            pltpu.SemaphoreType.DMA((FAR,)),
        ],
        24,
    )(own, other, attn, back_heads, near, in_hbm(far), inv)
    got = swap(other_grad)
    both = shape((CHIPS, 3 * HD + LAST, TOK), BF16)
    joined = call(join_kernel, both, [VM] * 3, 10**6, 10**6)(query_grad, own_grad, got)
    joined, stats = call(
        reduce_kernel,
        (both, shape((8, TOK), F32)),
        [VM, ANY],
        10**6,
        10**6,
        [pltpu.VMEM((CHIPS, LAST, TOK), BF16), pltpu.SemaphoreType.DMA],
        outs=(ANY, VM),
        aliases={1: 0},
    )(weight_parts, joined)
    grads = exchange(joined, "patch_0")
    rows = shape((1, FEAT, TOK), F32)
    query_out, key_out, value_out, weight_grad, loss = call(
        unpack_kernel,
        (rows, rows, rows, shape((ROWS, COLS), F32), shape((1, 1), F32)),
        [VM, VM],
        10**6,
        10**6,
    )(grads, stats)
    grads_out = (jnp.swapaxes(rows, 1, 2) for rows in (query_out, key_out, value_out))
    return *grads_out, weight_grad, loss[0, 0]


def solution(mesh):
    torus = Mesh(mesh.devices.reshape(4, 8, 8, 2), ("dp_0", "dp_1", "patch_0", "patch_1"))
    return jax.shard_map(
        local,
        mesh=torus,
        in_specs=(
            P(DP, PATCH, None),
            P(DP, PATCH, None),
            P(DP, PATCH, None),
            P(),
            P(DP, PATCH, None),
            P(DP),
            P(DP, PATCH),
        ),
        out_specs=(P(DP, PATCH, None), P(DP, PATCH, None), P(DP, PATCH, None), P(PATCH, DP), P()),
        check_vma=False,
    )
```

```python
import math

import jax
import jax.numpy as jnp
from jax import lax
from jax.experimental import pallas as pl
from jax.experimental.pallas import tpu as pltpu
from jax.sharding import Mesh
from jax.sharding import PartitionSpec as P


WIDTH = 1152
HEADS = 8
HD = 72
TOK = 128
FEAT = 576
SEQ = 2048
SAMPLES = 32
CHIPS = 8
PATCHES = 16
COLS = WIDTH // SAMPLES
ROWS = FEAT // PATCHES
HALF = FEAT // 2
STAT = COLS * HALF // TOK
PAD = 88
THIRD = ROWS // 3
LAST = 16
PAIR = WIDTH + HALF + 8
BUF = 3 * HD + 8
QB = 256
KEYS = 256
NEAR = 1
FAR = SEQ // 2 // QB - NEAR
NEG_LARGE = -1e30
SCALE = 1.0 / math.sqrt(HD)
EXP2_SCALE = SCALE * math.log2(math.e)
PATCH = ("patch_0", "patch_1")
DP = ("dp_0", "dp_1")
F32 = jnp.float32
BF16 = jnp.bfloat16

VM = pl.BlockSpec(memory_space=pltpu.VMEM)
SM = pl.BlockSpec(memory_space=pltpu.SMEM)
HB = pl.BlockSpec(memory_space=pltpu.HBM)
ANY = pl.BlockSpec(memory_space=pl.ANY)


def call(kernel, out_shape, in_specs, flops, nbytes, scratch=(), limit=16, outs=None, aliases=None):
    return pl.pallas_call(
        kernel,
        out_shape=out_shape,
        in_specs=in_specs,
        out_specs=outs if outs is not None else jax.tree.map(lambda _: VM, out_shape),
        scratch_shapes=list(scratch),
        input_output_aliases=aliases or {},
        cost_estimate=pl.CostEstimate(flops=flops, bytes_accessed=nbytes, transcendentals=0),
        compiler_params=pltpu.CompilerParams(vmem_limit_bytes=limit * 1024 * 1024),
    )


def dot(a, b, dims):
    return lax.dot_general(a, b, (dims, ((), ())), preferred_element_type=F32)


NN = ((1,), (0,))
NT = ((1,), (1,))


def pack_kernel(q_ref, k_ref, v_ref, seg_ref, out_ref, seg_sc, sems):
    copies = [
        pltpu.make_async_copy(ref, out_ref.at[:, at * HD : (at + 1) * HD, :], sems.at[at])
        for at, ref in enumerate((q_ref, k_ref, v_ref))
    ]
    copies.append(pltpu.make_async_copy(seg_ref, seg_sc, sems.at[3]))
    for copy in copies:
        copy.start()
    copies[3].wait()
    seg = jnp.broadcast_to(seg_sc[...].astype(F32), (8, TOK)).astype(BF16)
    for h in range(HEADS):
        out_ref[h, 3 * HD : BUF, :] = seg
    for copy in copies[:3]:
        copy.wait()


def group_rows(ref, chip, core, length):
    seg = ref[chip, 3 * HD : BUF, :].astype(F32)[0:1]
    at = (2 * chip + core) * TOK + lax.broadcasted_iota(jnp.int32, (1, TOK), 1)
    return jnp.where(at < length, seg, -1.0)


def forward_kernel(
    len_ref, own_ref, other_ref, attn_ref, near_ref, far_ref, inv_ref, key_sc, group_sc, value_sc, far_sc, sems, *score_refs
):
    core = lax.axis_index("patch_1")
    length = len_ref[0]
    own_groups = []
    copies = [pltpu.make_async_copy(far_sc.at[i], far_ref.at[i], sems.at[i]) for i in range(FAR)]
    for side, ref in enumerate((own_ref, other_ref)):
        for c in range(CHIPS):
            at = (side * CHIPS + c) * TOK
            key_sc[at : at + TOK, :] = ref[c, HD : 2 * HD, :].astype(F32).T.astype(BF16)
            value_sc[:, at : at + TOK] = ref[c, 2 * HD : 3 * HD, :]
            group = group_rows(ref, c, core if side == 0 else 1 - core, length)
            if side == 0:
                own_groups.append(group)
            group_sc[at : at + TOK, :] = jnp.broadcast_to(group, (TOK, TOK)).T
    order = (*range(NEAR, NEAR + FAR), *range(NEAR))
    pair = QB // TOK
    held = None
    for step in range(len(order) + 1):
        scores = score_refs[step % 2]
        if step < len(order):
            chips = range(order[step] * pair, (order[step] + 1) * pair)
            query = jnp.concatenate([own_ref[c, 0:HD, :] for c in chips], axis=1)
            group = jnp.concatenate([own_groups[c] for c in chips], axis=1)
            top = jnp.full((8, QB), NEG_LARGE, F32)
        if held is not None:
            b, held_scores, held_top = held
            weights_ref = near_ref.at[b] if b < NEAR else far_sc.at[b - NEAR]
            denom = jnp.zeros((8, QB), F32)
            accum = jnp.zeros((HD, QB), F32)
        for j in range(SEQ // KEYS):
            rows = slice(j * KEYS, (j + 1) * KEYS)
            if step < len(order):
                key_group = jnp.concatenate([group_sc[rows, :]] * pair, axis=1)
                masked = jnp.where(key_group == group, dot(key_sc[rows, :], query, NN), NEG_LARGE)
                scores[rows, :] = masked
                top = jnp.maximum(top, jnp.max(masked.reshape(KEYS // 8, 8, QB), axis=0))
            if held is not None:
                probs = jnp.exp2((held_scores[rows, :] - held_top) * EXP2_SCALE)
                denom = denom + jnp.sum(probs.reshape(KEYS // 8, 8, QB), axis=0)
                weights = probs.astype(BF16)
                weights_ref[rows, :] = weights
                accum = accum + dot(value_sc[:, rows], weights, NN)
        if held is not None:
            if b >= NEAR:
                copies[b - NEAR].start()
            inv = 1.0 / jnp.sum(denom, axis=0, keepdims=True)
            attn = (accum * inv).astype(BF16)
            inv_ref[b : b + 1, :] = inv
            for i in range(pair):
                attn_ref[b * pair + i] = attn[:, i * TOK : (i + 1) * TOK]
        if step < len(order):
            held = (order[step], scores, jnp.max(top, axis=0, keepdims=True))
    for copy in copies:
        copy.wait()


def high_low(value):
    high = value.astype(BF16).astype(F32)
    return high, value - high


def project_kernel(len_ref, attn_ref, weight_ref, target_ref, back_ref, out_ref, loss_ref):
    place = 2 * lax.axis_index("patch_0") + lax.axis_index("patch_1")
    attn = attn_ref[...].reshape(FEAT, TOK).astype(F32).T.astype(BF16)
    output = dot(attn, weight_ref[...], NN)
    at = place * TOK + lax.broadcasted_iota(jnp.int32, (TOK, WIDTH), 0)
    error = jnp.where(at < len_ref[0], output - target_ref[0].astype(F32), 0.0)
    grad_out = (2.0 * error).T.astype(BF16)
    back = dot(weight_ref[...], grad_out, NN).astype(BF16)
    for h in range(HEADS):
        back_ref[h] = back[h * HD : (h + 1) * HD, :]
    out_ref[...] = grad_out
    loss = jnp.sum(error * error, axis=0, keepdims=True)
    loss_ref[...] = sum(loss[:, i * TOK : (i + 1) * TOK] for i in range(WIDTH // TOK))


def pair_kernel(attn_ref, grad_ref, loss_ref, pair_ref, half_ref):
    first = lax.axis_index("patch_1") == 0
    wide = attn_ref[...].reshape(FEAT, TOK).astype(F32)
    sides = []
    for side in (0, 1):
        pieces = [wide[p * ROWS : (p + 1) * ROWS] for p in range(side, PATCHES, 2)]
        sides.append(jnp.concatenate(pieces, axis=0))
    half_ref[...] = jnp.where(first, sides[0], sides[1]).astype(BF16)
    stats = jnp.concatenate([*high_low(loss_ref[...]), jnp.zeros((6, TOK), F32)], axis=0)
    pair_ref[0:WIDTH, :] = grad_ref[...]
    pair_ref[WIDTH : WIDTH + HALF, :] = jnp.where(first, sides[1], sides[0]).astype(BF16)
    pair_ref[WIDTH + HALF : PAIR, :] = stats.astype(BF16)


def stat_rows(count, loss):
    upper = jnp.floor(count * (1.0 / 256.0))
    rows = [upper, count - 256.0 * upper, *high_low(loss), jnp.zeros((PAD - STAT - 4, TOK), F32)]
    return jnp.concatenate(rows, axis=0)


def stats_of(block):
    count = 256.0 * block[STAT : STAT + 1] + block[STAT + 1 : STAT + 2]
    return count, block[STAT + 2 : STAT + 3] + block[STAT + 3 : STAT + 4]


def weight_kernel(len_ref, mine_ref, got_ref, half_ref, out_ref, acc):
    left = jnp.concatenate([mine_ref[0:WIDTH, :], got_ref[0:WIDTH, :]], axis=1)
    right = jnp.concatenate([half_ref[...], got_ref[WIDTH : WIDTH + HALF, :]], axis=1)
    acc[:, 0:HALF] = dot(left, right, NT)
    stats = mine_ref[WIDTH + HALF : PAIR, :].astype(F32) + got_ref[WIDTH + HALF : PAIR, :].astype(F32)
    tail = stat_rows(jnp.full((1, TOK), len_ref[0].astype(F32)), stats[0:1] + stats[1:2])
    part = COLS // 4
    for d in range(SAMPLES):
        at = d * COLS
        rest = [acc[at + i * part : at + (i + 1) * part, 2 * TOK : HALF] for i in range(4)]
        block = [
            acc[at : at + COLS, 0:TOK],
            acc[at : at + COLS, TOK : 2 * TOK],
            jnp.concatenate(rest, axis=1),
            tail,
        ]
        out_ref[d] = jnp.concatenate(block, axis=0).astype(BF16)


def backward_kernel(
    own_ref,
    other_ref,
    attn_ref,
    back_ref,
    near_ref,
    far_ref,
    inv_ref,
    query_out,
    own_out,
    other_out,
    value_sc,
    key_sc,
    key_acc,
    value_acc,
    far_sc,
    sems,
):
    copies = [pltpu.make_async_copy(far_ref.at[i], far_sc.at[i], sems.at[i]) for i in range(FAR)]
    for copy in copies:
        copy.start()
    for side, ref in enumerate((own_ref, other_ref)):
        for c in range(CHIPS):
            at = (side * CHIPS + c) * TOK
            value_sc[at : at + TOK, :] = ref[c, 2 * HD : 3 * HD, :].astype(F32).T.astype(BF16)
            key_sc[:, at : at + TOK] = ref[c, HD : 2 * HD, :]
    for b in range(SEQ // 2 // QB):
        pair = QB // TOK
        chips = range(b * pair, (b + 1) * pair)
        query = jnp.concatenate([own_ref[c, 0:HD, :] for c in chips], axis=1)
        attn = jnp.concatenate([attn_ref[c] for c in chips], axis=1)
        back = jnp.concatenate([back_ref[c] for c in chips], axis=1)
        back = (back.astype(F32) * inv_ref[b : b + 1, :]).astype(BF16)
        delta = jnp.sum(back.astype(F32) * attn.astype(F32), axis=0, keepdims=True)
        if b == NEAR:
            for copy in copies:
                copy.wait()
        probs = near_ref[b] if b < NEAR else far_sc[b - NEAR]
        dprobs = dot(value_sc[...], back, NN)
        dscores = (probs.astype(F32) * (dprobs - delta)).astype(BF16)
        query_grad = dot(key_sc[...], dscores, NN).astype(BF16)
        for i, c in enumerate(chips):
            query_out[c] = query_grad[:, i * TOK : (i + 1) * TOK]
        key_part = dot(query, dscores, NT)
        value_part = dot(back, probs, NT)
        if b == 0:
            key_acc[...] = key_part
            value_acc[...] = value_part
        else:
            key_acc[...] += key_part
            value_acc[...] += value_part
    for side, ref in enumerate((own_out, other_out)):
        for c in range(CHIPS):
            at = (side * CHIPS + c) * TOK
            ref[c, 0:HD, :] = key_acc[:, at : at + TOK].astype(BF16)
            ref[c, HD : 2 * HD, :] = value_acc[:, at : at + TOK].astype(BF16)


def join_kernel(query_ref, own_ref, other_ref, out_ref):
    out_ref[:, 0:HD, :] = query_ref[...]
    out_ref[:, HD : 3 * HD, :] = (own_ref[...].astype(F32) + other_ref[...].astype(F32)).astype(BF16)


def reduce_kernel(part_ref, join_ref, out_ref, stat_ref, last_sc, sem):
    del join_ref
    total = part_ref[0].astype(F32)
    for d in range(1, SAMPLES):
        total = total + part_ref[d].astype(F32)
    count, loss = stats_of(total)
    stat_ref[...] = jnp.broadcast_to(count, (8, TOK))
    rest = total[2 * COLS : STAT]
    width = HALF - 2 * TOK
    rest = jnp.concatenate([rest[:, i * width : (i + 1) * width] for i in range(4)], axis=0)
    rest = jnp.concatenate([rest, jnp.zeros((COLS, TOK - width), F32)], axis=1)
    block = jnp.concatenate([total[0:COLS], total[COLS : 2 * COLS], rest], axis=1)
    turned = jnp.concatenate([block, jnp.zeros((TOK - COLS, 3 * TOK), F32)], axis=0).T
    loss = jnp.concatenate([*high_low(loss), jnp.zeros((LAST - THIRD - 2, TOK), F32)], axis=0)
    for c in range(CHIPS):
        thirds = [turned[c * ROWS + i * THIRD : c * ROWS + (i + 1) * THIRD, 0:COLS] for i in range(3)]
        rows = jnp.concatenate([*thirds, jnp.zeros((THIRD, TOK - 3 * COLS), F32)], axis=1)
        last_sc[c] = jnp.concatenate([rows, loss], axis=0).astype(BF16)
    copy = pltpu.make_async_copy(last_sc, out_ref.at[:, 3 * HD : 3 * HD + LAST, :], sem)
    copy.start()
    copy.wait()


def unpack_kernel(
    rows_ref, stat_ref, query_ref, key_ref, value_ref, weight_ref, loss_ref, grad_sc, sems
):
    copies = []
    count = stat_ref[0:1, :]
    ratio = float(SAMPLES * SEQ) / count
    for at, (ref, factor) in enumerate(((query_ref, SCALE), (key_ref, SCALE), (value_ref, 1.0))):
        for h in range(HEADS):
            rows = rows_ref[h, at * HD : (at + 1) * HD, :].astype(F32)
            grad_sc[at, h * HD : (h + 1) * HD, :] = rows * (ratio * factor)
        copies.append(pltpu.make_async_copy(grad_sc.at[at], ref.at[0], sems.at[at]))
        copies[at].start()
    total = sum(rows_ref[c, 3 * HD : 3 * HD + LAST, :].astype(F32) for c in range(CHIPS))
    scaled = total * (ratio / SEQ)
    thirds = [scaled[0:THIRD, i * COLS : (i + 1) * COLS] for i in range(3)]
    weight_ref[...] = jnp.concatenate(thirds, axis=0)
    loss = jnp.sum(total[THIRD : THIRD + 1] + total[THIRD + 1 : THIRD + 2], axis=1, keepdims=True)
    loss_ref[...] = loss / (count[:, 0:1] * WIDTH)
    for copy in copies:
        copy.wait()


def in_hbm(value):
    return pltpu.with_memory_space_constraint(value, pltpu.HBM)


def exchange(value, axis):
    return lax.all_to_all(value, axis, 0, 0, tiled=True)


def swap(value):
    return lax.ppermute(value, "patch_1", [(0, 1), (1, 0)])


def shape(dims, dtype):
    return jax.ShapeDtypeStruct(dims, dtype)


def local(query_rows, key_rows, value_rows, out_weight, target, lengths, segments):
    buffer = shape((CHIPS, BUF, TOK), BF16)
    heads = shape((CHIPS, HD, TOK), BF16)
    turned = [
        in_hbm(jnp.swapaxes(rows, 1, 2).reshape(HEADS, HD, TOK))
        for rows in (query_rows, key_rows, value_rows)
    ]
    packed = call(
        pack_kernel,
        buffer,
        [HB] * 4,
        10**6,
        10**6,
        [pltpu.VMEM((1, TOK), jnp.int32), pltpu.SemaphoreType.DMA((4,))],
        2,
    )(*turned, in_hbm(segments))
    own = exchange(packed, "patch_0")
    other = swap(own)
    blocks = SEQ // 2 // QB
    attn, near, far, inv = call(
        forward_kernel,
        (heads, shape((NEAR, SEQ, QB), BF16), pltpu.HBM((FAR, SEQ, QB), BF16), shape((blocks, QB), F32)),
        [SM, VM, VM],
        4 * HD * SEQ * SEQ // 2,
        6 * 10**6,
        [
            pltpu.VMEM((SEQ, HD), BF16),
            pltpu.VMEM((SEQ, TOK), F32),
            pltpu.VMEM((HD, SEQ), BF16),
            pltpu.VMEM((FAR, SEQ, QB), BF16),
            pltpu.SemaphoreType.DMA((FAR,)),
            pltpu.VMEM((SEQ, QB), F32),
            pltpu.VMEM((SEQ, QB), F32),
        ],
        24,
        (VM, VM, HB, VM),
    )(lengths, own, other)
    attn_rows = exchange(attn, "patch_0")
    back, grad_out, loss_part = call(
        project_kernel,
        (heads, shape((WIDTH, TOK), BF16), shape((1, TOK), F32)),
        [SM, VM, VM, VM],
        4 * TOK * FEAT * WIDTH,
        3 * 10**6,
    )(lengths, attn_rows, out_weight, target)
    back_heads = exchange(back, "patch_0")
    mine, half = call(
        pair_kernel, (shape((PAIR, TOK), BF16), shape((HALF, TOK), BF16)), [VM] * 3, 10**6, 10**6
    )(attn_rows, grad_out, loss_part)
    got_pair = swap(mine)
    weight_part = call(
        weight_kernel,
        shape((SAMPLES, PAD, TOK), BF16),
        [SM, VM, VM, VM],
        2 * TOK * FEAT * WIDTH,
        3 * 10**6,
        [pltpu.VMEM((WIDTH, 3 * TOK), F32)],
    )(lengths, mine, got_pair, half)
    weight_parts = exchange(weight_part, DP)
    pair = shape((CHIPS, 2 * HD, TOK), BF16)
    query_grad, own_grad, other_grad = call(
        backward_kernel,
        (heads, pair, pair),
        [VM, VM, VM, VM, VM, HB, VM],
        8 * HD * SEQ * SEQ // 2,
        6 * 10**6,
        [
            pltpu.VMEM((SEQ, HD), BF16),
            pltpu.VMEM((HD, SEQ), BF16),
            pltpu.VMEM((HD, SEQ), F32),
            pltpu.VMEM((HD, SEQ), F32),
            pltpu.VMEM((FAR, SEQ, QB), BF16),
            pltpu.SemaphoreType.DMA((FAR,)),
        ],
        24,
    )(own, other, attn, back_heads, near, in_hbm(far), inv)
    got = swap(other_grad)
    both = shape((CHIPS, 3 * HD + LAST, TOK), BF16)
    joined = call(join_kernel, both, [VM] * 3, 10**6, 10**6)(query_grad, own_grad, got)
    joined, stats = call(
        reduce_kernel,
        (both, shape((8, TOK), F32)),
        [VM, ANY],
        10**6,
        10**6,
        [pltpu.VMEM((CHIPS, LAST, TOK), BF16), pltpu.SemaphoreType.DMA],
        outs=(ANY, VM),
        aliases={1: 0},
    )(weight_parts, joined)
    grads = exchange(joined, "patch_0")
    rows = pltpu.HBM((1, FEAT, TOK), F32)
    query_out, key_out, value_out, weight_grad, loss = call(
        unpack_kernel,
        (rows, rows, rows, shape((ROWS, COLS), F32), shape((1, 1), F32)),
        [VM, VM],
        10**6,
        10**6,
        [pltpu.VMEM((3, FEAT, TOK), F32), pltpu.SemaphoreType.DMA((3,))],
        outs=(HB, HB, HB, VM, VM),
    )(grads, stats)
    grads_out = (jnp.swapaxes(rows, 1, 2) for rows in (query_out, key_out, value_out))
    return *grads_out, weight_grad, loss[0, 0]


def solution(mesh):
    torus = Mesh(mesh.devices.reshape(4, 8, 8, 2), ("dp_0", "dp_1", "patch_0", "patch_1"))
    return jax.shard_map(
        local,
        mesh=torus,
        in_specs=(
            P(DP, PATCH, None),
            P(DP, PATCH, None),
            P(DP, PATCH, None),
            P(),
            P(DP, PATCH, None),
            P(DP),
            P(DP, PATCH),
        ),
        out_specs=(P(DP, PATCH, None), P(DP, PATCH, None), P(DP, PATCH, None), P(PATCH, DP), P()),
        check_vma=False,
    )
```
